32 devices in a mesh: seq: 4 (over y, core), span: 8 (over z, x).
Axes of the slice: x: 2, y: 2, z: 4, core: 2. Of those that a mesh axis runs over, the one named last changes fastest.
Arguments:
- queries: bfloat16 [8, 512, 1536], P('span', 'seq'), may hold values from -6 to 6
- key_head_matrix: bfloat16 [8, 512, 512], P('span', 'seq'), may hold values from -6 to 6
- value_head_matrix: bfloat16 [8, 512, 512], P('span', 'seq'), may hold values from -6 to 6
- attn_output: bfloat16 [8, 512, 1536], P('span', 'seq'), may hold values from -6 to 6
- out_grad: bfloat16 [8, 512, 1536], P('span', 'seq'), may hold values from -6 to 6
Outputs:
- query_grad: bfloat16 [8, 512, 1536], P('span', 'seq')
- key_grad: bfloat16 [8, 512, 512], P('span', 'seq')
- value_grad: bfloat16 [8, 512, 512], P('span', 'seq')
The draws below stay inside these ranges and needn't reach their ends.
All inputs are finite; a program needn't handle non-finite values.
Results may differ from the reference program's by a relative error of at most 0.005.
Values may be sent and summed in bfloat16 or wider, within the bound.
A program may use at most 64 MiB of HBM per device.

```python
import math
import jax
import jax.numpy as jnp
from jax import lax

HEAD_WIDTH = 64
KEY_HEADS = 8
QUERY_PER_KEY = 3
HQ = 24
BLOCK_TOKENS = 512
SEQUENCE_BLOCKS = 8


def draw_queries(key, part):
    random_seed_key = jax.random.fold_in(key, 1)
    value_rows = jax.random.truncated_normal(random_seed_key, -6.0, 6.0, (SEQUENCE_BLOCKS, BLOCK_TOKENS, HQ * HEAD_WIDTH), jnp.float32)
    return value_rows.astype(jnp.bfloat16)


def draw_key_head_matrix(key, part):
    random_seed_key = jax.random.fold_in(key, 2)
    value_rows = jax.random.truncated_normal(random_seed_key, -6.0, 6.0, (SEQUENCE_BLOCKS, BLOCK_TOKENS, KEY_HEADS * HEAD_WIDTH), jnp.float32)
    return value_rows.astype(jnp.bfloat16)


def shard_levels(own_key, shape, split, smallest, largest):
    gain = 1.0
    for position, blocks in split:
        heights = jax.random.uniform(jax.random.fold_in(jax.random.fold_in(own_key, 6), position), (blocks,), jnp.float32, smallest / len(split), largest / len(split))
        gain = gain * jnp.repeat(jnp.exp(heights), shape[position] // blocks).reshape((-1,) + (1,) * (len(shape) - 1 - position))
    return gain


def bell_draw(own_key, extent, scale, limit, split=(), held_as=jnp.bfloat16):
    values = jax.random.normal(own_key, extent, jnp.float32) * scale
    if len(split) > 0:
        values = shard_levels(own_key, extent, split, -0.22, 0.18) * values
    return jnp.clip(values, min=-limit, max=limit).astype(held_as)


def setup_inputs(seed: int = 0) -> dict:
    key_of = jax.random.split(jax.random.key(seed), 6)
    queries = draw_queries(jax.random.fold_in(key_of[5], 71), 0)
    key_head_matrix = draw_key_head_matrix(jax.random.fold_in(key_of[5], 71), 0)
    value_head_matrix = bell_draw(key_of[2], (SEQUENCE_BLOCKS, BLOCK_TOKENS, KEY_HEADS * HEAD_WIDTH), 1.0, 6.0, ((0, 8), (1, 4)))
    attn_output = bell_draw(key_of[3], (SEQUENCE_BLOCKS, BLOCK_TOKENS, HQ * HEAD_WIDTH), 1.0, 6.0, ((0, 8), (1, 4)))
    out_grad = bell_draw(key_of[4], (SEQUENCE_BLOCKS, BLOCK_TOKENS, HQ * HEAD_WIDTH), 1.0, 6.0, ((0, 8), (1, 4)))
    return {"queries": queries, "key_head_matrix": key_head_matrix, "value_head_matrix": value_head_matrix, "attn_output": attn_output, "out_grad": out_grad}


NEG_LARGE = -1e+30

def head_grads(running, inputs):
    query_head, key_head, value_head, output_head, grad_head = inputs
    sequence_length = query_head.shape[0]
    scaling = 1.0 / math.sqrt(HEAD_WIDTH)
    positions = lax.iota(jnp.int32, sequence_length)
    allowed = positions[None, :] <= positions[:, None]
    scores = jnp.dot(query_head, key_head.T, preferred_element_type=jnp.float32) * scaling
    row_max = lax.optimization_barrier(jnp.max(jnp.where(allowed, scores, NEG_LARGE), axis=1))
    row_sum = lax.optimization_barrier(jnp.sum(jnp.where(allowed, jnp.exp(scores - row_max[:, None]), 0.0), axis=1))
    log_norm = row_max + jnp.log(row_sum)
    prob_weights = jnp.where(allowed, jnp.exp(scores - log_norm[:, None]), 0.0)
    row_delta = lax.optimization_barrier(jnp.sum(grad_head.astype(jnp.float32) * output_head.astype(jnp.float32), axis=1))
    prob_grad = jnp.dot(grad_head, value_head.T, preferred_element_type=jnp.float32)
    score_low = (prob_weights * (prob_grad - row_delta[:, None])).astype(jnp.bfloat16)
    prob_low = prob_weights.astype(jnp.bfloat16)
    query_part = scaling * jnp.dot(score_low, key_head, preferred_element_type=jnp.float32)
    key_piece = scaling * jnp.dot(score_low.T, query_head, preferred_element_type=jnp.float32)
    value_piece = jnp.dot(prob_low.T, grad_head, preferred_element_type=jnp.float32)
    return (running, (query_part, key_piece, value_piece))

def reference(queries, key_head_matrix, value_head_matrix, attn_output, out_grad):
    sequence_length = SEQUENCE_BLOCKS * BLOCK_TOKENS

    def each_head_share(source, head_count):
        return jnp.transpose(source.reshape(sequence_length, head_count, HEAD_WIDTH), (1, 0, 2))
    key_complete = jnp.repeat(each_head_share(key_head_matrix, KEY_HEADS), QUERY_PER_KEY, axis=0)
    value_complete = jnp.repeat(each_head_share(value_head_matrix, KEY_HEADS), QUERY_PER_KEY, axis=0)
    start_state = jnp.zeros((), jnp.float32)
    final_state, head_results = lax.scan(head_grads, start_state, (each_head_share(queries, HQ), key_complete, value_complete, each_head_share(attn_output, HQ), each_head_share(out_grad, HQ)))
    query_part, key_piece, value_piece = head_results
    query_out = jnp.transpose(query_part, (1, 0, 2)).reshape(SEQUENCE_BLOCKS, BLOCK_TOKENS, HQ * HEAD_WIDTH).astype(jnp.bfloat16)
    key_total = lax.optimization_barrier(jnp.sum(key_piece.reshape(KEY_HEADS, QUERY_PER_KEY, sequence_length, HEAD_WIDTH), axis=1))
    value_total = lax.optimization_barrier(jnp.sum(value_piece.reshape(KEY_HEADS, QUERY_PER_KEY, sequence_length, HEAD_WIDTH), axis=1))
    key_result = jnp.transpose(key_total, (1, 0, 2)).reshape(SEQUENCE_BLOCKS, BLOCK_TOKENS, KEY_HEADS * HEAD_WIDTH).astype(jnp.bfloat16)
    value_result = jnp.transpose(value_total, (1, 0, 2)).reshape(SEQUENCE_BLOCKS, BLOCK_TOKENS, KEY_HEADS * HEAD_WIDTH).astype(jnp.bfloat16)
    return (query_out, key_result, value_result)
```

```python
import functools
import math

import jax
import jax.numpy as jnp
from jax import lax
from jax.experimental import pallas as pl
from jax.experimental.pallas import tpu as pltpu
from jax.sharding import PartitionSpec as P

HEAD_WIDTH = 64
PAIR = 2 * HEAD_WIDTH
QUERY_PER_KEY = 3
NEG_LARGE = -1e30
MESH = pl.DeviceIdType.MESH
LOG2E = math.log2(math.e)
SCORE_BYTES = 26 * 2**20


def dot(a, b, contract):
    return lax.dot_general(a, b, ((contract[:1], contract[1:]), ((), ())), preferred_element_type=jnp.float32)


def kernel(kv_heads, resident, q_ref, k_ref, v_ref, o_ref, g_ref, dq_out, dk_out, dv_out,
           qg_send, kv_send, dl_send, qg_in, kv_in, dl_in, q_pad, g_pad, dl_row, s_ref, m_ref, l_ref, dqt_ref,
           acc_ref, dq_send, dq_in, part_ref, red_in, fin_ref, dkv_in,
           qg_s, qg_r, kv_s, kv_r, dl_s, dl_r, side_s, hand_s, dq_s, dq_r, red_s, red_r, fin_s, fin_r):
    seq_count = lax.axis_size("seq")
    seq = lax.axis_index("seq")
    span = lax.axis_index("span")
    heads = QUERY_PER_KEY
    spread = lax.axis_size("span") // kv_heads
    splits = spread * seq_count
    tokens = q_ref.shape[1]
    per = kv_heads // 2
    chunk = per * tokens
    top = 2 * splits - 1
    me = span * seq_count + seq
    my_head = span // spread
    my_split = lax.rem(span, spread) * seq_count + seq
    scaling = 1.0 / math.sqrt(HEAD_WIDTH)
    factor = scaling * LOG2E

    def rank_of(split):
        return 2 * lax.rem(split, splits // 2) + split // (splits // 2)

    def split_of(rank):
        return lax.rem(rank, 2) * (splits // 2) + rank // 2

    my_rank = rank_of(my_split)
    my_chunk = me // per
    my_kind = jnp.where(my_chunk < splits, 0, 1)
    my_sub = lax.rem(me, per)
    q_split = split_of(jnp.where(my_chunk < splits, my_chunk, top - my_chunk))

    def chunk_of(kind):
        return top - my_rank if kind else my_rank

    def member(head, split):
        return {"seq": lax.rem(split, seq_count), "span": head * spread + split // seq_count}

    def source(piece):
        return {"seq": lax.rem(piece, seq_count), "span": piece // seq_count}

    def remote(src, dst, send, recv, device):
        return pltpu.make_async_remote_copy(src_ref=src, dst_ref=dst, send_sem=send, recv_sem=recv,
                                            device_id=device, device_id_type=MESH)

    def other(mine, fn_other, fn_mine):
        @pl.when(mine)
        def _():
            fn_mine()

        @pl.when(jnp.logical_not(mine))
        def _():
            fn_other()

    def qg_copy(h, j):
        return remote(qg_send.at[h, j], qg_in.at[my_kind, j, my_sub], qg_s.at[h, j], qg_r.at[my_kind, j, my_sub],
                      member(h, q_split))

    def qg_own(h, j):
        return pltpu.make_async_copy(qg_send.at[h, j], qg_in.at[my_kind, j, my_sub], qg_s.at[h, j])

    def dl_copy(h):
        return remote(dl_send.at[h], dl_in.at[my_kind, my_sub], dl_s.at[h], dl_r.at[my_kind, my_sub],
                      member(h, q_split))

    def dl_own(h):
        return pltpu.make_async_copy(dl_send.at[h], dl_in.at[my_kind, my_sub], dl_s.at[h])

    def q_mine(h):
        return jnp.logical_and(h == my_head, q_split == my_split)

    def kv_copy(h):
        return remote(kv_send.at[h], kv_in.at[me], kv_s.at[h], kv_r.at[me], member(h, my_split))

    def kv_own(h):
        return pltpu.make_async_copy(kv_send.at[h], kv_in.at[me], kv_s.at[h])

    twin = my_split + 1 - 2 * lax.rem(my_split, 2)

    def step_split(k):
        return lax.rem(my_split + 2 * k, splits)

    def hand_copy(i, k):
        piece = i * splits + my_split
        return remote(kv_in.at[piece], kv_in.at[piece], hand_s.at[k, i], kv_r.at[piece],
                      member(my_head, step_split(k)))

    def twin_copy(i, k):
        piece = i * splits + step_split(k)
        return remote(kv_in.at[piece], kv_in.at[piece], side_s.at[k, i], kv_r.at[piece], member(my_head, twin))

    def kv_wait(piece):
        remote(kv_in.at[piece], kv_in.at[piece], kv_s.at[0], kv_r.at[piece], member(my_head, twin)).wait_recv()

    def dq_copy(kind, j, sub):
        piece = chunk_of(kind) * per + sub
        return remote(dq_send.at[kind, j, sub], dq_in.at[my_head, j], dq_s.at[kind, j, sub], dq_r.at[my_head, j],
                      source(piece))

    def dq_own(kind, j, sub):
        return pltpu.make_async_copy(dq_send.at[kind, j, sub], dq_in.at[my_head, j], dq_s.at[kind, j, sub])

    def red_copy(c, sub):
        piece = c * per + sub
        to = lax.rem(piece, splits)
        return remote(part_ref.at[piece], red_in.at[my_split, piece // splits], red_s.at[piece],
                      red_r.at[my_split, piece // splits], member(my_head, to))

    def fin_copy(i):
        return remote(fin_ref.at[i], dkv_in.at[my_head], fin_s.at[i], fin_r.at[my_head],
                      source(i * splits + my_split))

    def fin_own(i):
        return pltpu.make_async_copy(fin_ref.at[i], dkv_in.at[my_head], fin_s.at[i])

    for h in range(kv_heads):
        at = slice(h * HEAD_WIDTH, (h + 1) * HEAD_WIDTH)
        kv_send[h] = jnp.concatenate([k_ref[0, :, at], v_ref[0, :, at]], axis=1)
    for h in range(kv_heads):
        other(h == my_head, lambda: kv_copy(h).start(), lambda: kv_own(h).start())
    for j in range(heads):
        for h in range(kv_heads):
            one = h * heads + j
            at = slice(one * HEAD_WIDTH, (one + 1) * HEAD_WIDTH)
            qg_send[h, j] = jnp.concatenate([q_ref[0, :, at], g_ref[0, :, at]], axis=1)
        for h in range(kv_heads):
            other(q_mine(h), lambda: qg_copy(h, j).start(), lambda: qg_own(h, j).start())
    product = o_ref[0].astype(jnp.float32) * g_ref[0].astype(jnp.float32)
    high = product.astype(jnp.bfloat16)
    low = (product - high.astype(jnp.float32)).astype(jnp.bfloat16)
    wide = kv_heads * heads * HEAD_WIDTH
    row = lax.broadcasted_iota(jnp.int32, (kv_heads * 8, wide), 0)
    column = lax.broadcasted_iota(jnp.int32, (kv_heads * 8, wide), 1) // HEAD_WIDTH
    ones = jnp.where(row == (column // heads) * 8 + lax.rem(column, heads), 1.0, 0.0).astype(jnp.bfloat16)
    dl_send[...] = (dot(ones, high, (1, 1)) + dot(ones, low, (1, 1))).reshape(kv_heads, 8, tokens)
    for h in range(kv_heads):
        other(q_mine(h), lambda: dl_copy(h).start(), lambda: dl_own(h).start())

    def clear(b, _):
        acc_ref[b] = jnp.zeros((chunk, PAIR), jnp.float32)
        return 0

    lax.fori_loop(0, 2 * splits, clear, 0)

    def hand_on(i, _):
        piece = i * splits + my_split
        other(piece == me, lambda: kv_wait(piece), lambda: kv_own(my_head).wait())
        twin_copy(i, 0).start()
        for k in range(1, splits // 2):
            hand_copy(i, k).start()
        return 0

    lax.fori_loop(0, kv_heads, hand_on, 0)

    def pass_on(i, _):
        for k in range(1, splits // 2):
            kv_wait(i * splits + step_split(k))
            twin_copy(i, k).start()
        return 0

    lax.fori_loop(0, kv_heads, pass_on, 0)

    def twin_wait(i, _):
        for k in range(splits // 2):
            kv_wait(i * splits + lax.rem(twin + 2 * k, splits))
        return 0

    lax.fori_loop(0, kv_heads, twin_wait, 0)

    lane = lax.broadcasted_iota(jnp.int32, (1, PAIR), 1)

    def kv_block(b):
        return kv_in[pl.ds(b * per, per)].reshape(chunk, PAIR)

    def hide(s):
        k_pos = lax.broadcasted_iota(jnp.int32, (chunk, chunk), 0)
        q_pos = lax.broadcasted_iota(jnp.int32, (chunk, chunk), 1)
        return jnp.where(k_pos <= q_pos, s, NEG_LARGE)

    def scores(b, j, last):
        s = dot(kv_block(b), q_pad[j], (1, 1))
        return hide(s) if last else s

    for kind in range(2):
        c_q = chunk_of(kind)
        for j in range(heads):
            for sub in range(per):
                mine = c_q * per + sub == me
                landing = qg_in.at[kind, j, sub]
                other(mine,
                      lambda: remote(landing, landing, qg_s.at[0, j], qg_r.at[kind, j, sub],
                                     member(my_head, twin)).wait_recv(),
                      lambda: qg_own(my_head, j).wait())
                if j == 0:
                    small = dl_in.at[kind, sub]
                    other(mine,
                          lambda: remote(small, small, dl_s.at[0], dl_r.at[kind, sub],
                                         member(my_head, twin)).wait_recv(),
                          lambda: dl_own(my_head).wait())
            both = qg_in[kind, j].reshape(chunk, PAIR)
            q_pad[j] = jnp.where(lane < HEAD_WIDTH, both, jnp.zeros_like(both))
            g_pad[j] = jnp.where(lane < HEAD_WIDTH, jnp.zeros_like(both), both)
            for sub in range(per):
                dl_row[j, :, sub * tokens:(sub + 1) * tokens] = dl_in[kind, sub, pl.ds(j, 1), :]
            dqt_ref[j] = jnp.zeros((HEAD_WIDTH, chunk), jnp.float32)
            m_ref[j] = jnp.full((1, chunk), NEG_LARGE, jnp.float32)
            l_ref[j] = jnp.zeros((1, chunk), jnp.float32)

            def block(b, last):
                s = scores(b, j, last)
                if resident:
                    s_ref[b * heads + j] = s
                m_old = m_ref[j]
                m_new = jnp.maximum(m_old, jnp.max(s, axis=0, keepdims=True))
                e = jnp.exp2((s - m_new) * factor)
                l_ref[j] = l_ref[j] * jnp.exp2((m_old - m_new) * factor) + jnp.sum(e, axis=0, keepdims=True)
                m_ref[j] = m_new
                return 0

            lax.fori_loop(0, c_q, lambda b, _: block(b, False), 0)
            block(c_q, True)
            m_ref[j] = m_ref[j] * factor + jnp.log2(l_ref[j])

        def grads(b, last):
            kv = kv_block(b)
            total = jnp.zeros((chunk, PAIR), jnp.float32)
            for j in range(heads):
                s = s_ref[b * heads + j] if resident else scores(b, j, last)
                p = jnp.exp2(s * factor - m_ref[j])
                dp = dot(kv, g_pad[j], (1, 1))
                ds = (p * (dp - dl_row[j])).astype(jnp.bfloat16)
                total += dot(ds, q_pad[j], (1, 0)) + dot(p.astype(jnp.bfloat16), g_pad[j], (1, 0))
                dqt_ref[j] += dot(kv[:, :HEAD_WIDTH].T, ds, (1, 0))
            acc_ref[b] += total

        def hand_out(b):
            done = acc_ref[b] * jnp.where(lane < HEAD_WIDTH, scaling, 1.0)
            part_ref[pl.ds(b * per, per)] = done.astype(jnp.bfloat16).reshape(per, tokens, PAIR)
            for sub in range(per):
                @pl.when(lax.rem(b * per + sub, splits) != my_split)
                def _():
                    red_copy(b, sub).start()

        def reduce(b):
            for sub in range(per):
                piece = b * per + sub

                @pl.when(lax.rem(piece, splits) == my_split)
                def _():
                    i = piece // splits
                    at = pl.ds(pl.multiple_of(sub * tokens, tokens), tokens)

                    def add(f, _):
                        @pl.when(jnp.logical_and(f != my_split, top - rank_of(f) >= b))
                        def _():
                            landing = red_in.at[f, i]
                            remote(landing, landing, red_s.at[0], red_r.at[f, i], member(my_head, twin)).wait_recv()
                            acc_ref[b, at, :] += red_in[f, i].astype(jnp.float32) * jnp.where(
                                lane < HEAD_WIDTH, 1.0 / scaling, 1.0)
                        return 0

                    lax.fori_loop(0, splits, add, 0)
                    fin_ref[i] = (acc_ref[b, at, :] * jnp.where(lane < HEAD_WIDTH, scaling, 1.0)).astype(jnp.bfloat16)
                    other(piece == me, lambda: fin_copy(i).start(), lambda: fin_own(i).start())

        if kind == 0:
            lax.fori_loop(0, c_q, lambda b, _: (grads(b, False), 0)[1], 0)
            grads(c_q, True)
        else:
            def sweep(t, _):
                b = top - t

                @pl.when(b < c_q)
                def _():
                    grads(b, False)

                @pl.when(b == c_q)
                def _():
                    grads(b, True)

                @pl.when(b <= c_q)
                def _():
                    hand_out(b)

                @pl.when(t > 0)
                def _():
                    reduce(b + 1)
                return 0

            lax.fori_loop(0, top + 1, sweep, 0)

        for j in range(heads):
            for sub in range(per):
                part = dqt_ref[j, :, sub * tokens:(sub + 1) * tokens] * scaling
                dq_send[kind, j, sub] = part.astype(jnp.bfloat16)
        for j in range(heads):
            for sub in range(per):
                other(c_q * per + sub == me, lambda: dq_copy(kind, j, sub).start(),
                      lambda: dq_own(kind, j, sub).start())
    reduce(0)

    for h in range(kv_heads):
        for j in range(heads):
            mine = q_mine(h)
            landing = dq_in.at[h, j]
            other(mine,
                  lambda: remote(landing, landing, dq_s.at[0, j, 0], dq_r.at[h, j], member(my_head, twin)).wait_recv(),
                  lambda: dq_own(my_kind, j, my_sub).wait())
    dq_out[0] = dq_in[...].reshape(kv_heads * heads * HEAD_WIDTH, tokens).T
    for h in range(kv_heads):
        landing = dkv_in.at[h]
        other(h == my_head,
              lambda: remote(landing, landing, fin_s.at[0], fin_r.at[h], member(my_head, twin)).wait_recv(),
              lambda: fin_own(my_head).wait())
    for h in range(0, kv_heads, 2):
        at = slice(h * HEAD_WIDTH, (h + 2) * HEAD_WIDTH)
        dk_out[0, :, at] = jnp.concatenate([dkv_in[h, :, :HEAD_WIDTH], dkv_in[h + 1, :, :HEAD_WIDTH]], axis=1)
        dv_out[0, :, at] = jnp.concatenate([dkv_in[h, :, HEAD_WIDTH:], dkv_in[h + 1, :, HEAD_WIDTH:]], axis=1)

    for h in range(kv_heads):
        @pl.when(h != my_head)
        def _():
            kv_copy(h).wait_send()

        @pl.when(jnp.logical_not(q_mine(h)))
        def _():
            dl_copy(h).wait_send()
            for j in range(heads):
                qg_copy(h, j).wait_send()

    def sent(i, _):
        for k in range(splits // 2):
            twin_copy(i, k).wait_send()
            if k:
                hand_copy(i, k).wait_send()

        @pl.when(i != my_head)
        def _():
            fin_copy(i).wait_send()
        return 0

    lax.fori_loop(0, kv_heads, sent, 0)
    for kind in range(2):
        for j in range(heads):
            for sub in range(per):
                @pl.when(chunk_of(kind) * per + sub != me)
                def _():
                    dq_copy(kind, j, sub).wait_send()

    def red_sent(b, _):
        for sub in range(per):
            @pl.when(lax.rem(b * per + sub, splits) != my_split)
            def _():
                red_copy(b, sub).wait_send()
        return 0

    lax.fori_loop(0, chunk_of(1) + 1, red_sent, 0)


def vmem(count):
    return [pl.BlockSpec(memory_space=pltpu.VMEM)] * count


def per_device(queries, key_head_matrix, value_head_matrix, attn_output, out_grad):
    seq_count = lax.axis_size("seq")
    tokens = queries.shape[1]
    kv_heads = key_head_matrix.shape[2] // HEAD_WIDTH
    splits = lax.axis_size("span") // kv_heads * seq_count
    pieces = kv_heads * splits
    heads = QUERY_PER_KEY
    per = kv_heads // 2
    chunk = per * tokens
    count = heads * 2 * splits
    resident = count * chunk * chunk * 4 <= SCORE_BYTES
    dma = pltpu.SemaphoreType.DMA
    low, full = jnp.bfloat16, jnp.float32
    return pl.pallas_call(
        functools.partial(kernel, kv_heads, resident),
        out_shape=(
            jax.ShapeDtypeStruct(queries.shape, low),
            jax.ShapeDtypeStruct(key_head_matrix.shape, low),
            jax.ShapeDtypeStruct(value_head_matrix.shape, low),
        ),
        in_specs=vmem(5),
        out_specs=tuple(vmem(3)),
        scratch_shapes=[
            pltpu.VMEM((kv_heads, heads, tokens, PAIR), low),
            pltpu.VMEM((kv_heads, tokens, PAIR), low),
            pltpu.VMEM((kv_heads, 8, tokens), full),
            pltpu.VMEM((2, heads, per, tokens, PAIR), low),
            pltpu.VMEM((pieces, tokens, PAIR), low),
            pltpu.VMEM((2, per, 8, tokens), full),
            pltpu.VMEM((heads, chunk, PAIR), low),
            pltpu.VMEM((heads, chunk, PAIR), low),
            pltpu.VMEM((heads, 1, chunk), full),
            pltpu.VMEM((count, chunk, chunk) if resident else (1, 8, chunk), full),
            pltpu.VMEM((heads, 1, chunk), full),
            pltpu.VMEM((heads, 1, chunk), full),
            pltpu.VMEM((heads, HEAD_WIDTH, chunk), full),
            pltpu.VMEM((2 * splits, chunk, PAIR), full),
            pltpu.VMEM((2, heads, per, HEAD_WIDTH, tokens), low),
            pltpu.VMEM((kv_heads, heads, HEAD_WIDTH, tokens), low),
            pltpu.VMEM((pieces, tokens, PAIR), low),
            pltpu.VMEM((splits, kv_heads, tokens, PAIR), low),
            pltpu.VMEM((kv_heads, tokens, PAIR), low),
            pltpu.VMEM((kv_heads, tokens, PAIR), low),
            dma((kv_heads, heads)),
            dma((2, heads, per)),
            dma((kv_heads,)),
            dma((pieces,)),
            dma((kv_heads,)),
            dma((2, per)),
            dma((splits // 2, kv_heads)),
            dma((splits // 2, kv_heads)),
            dma((2, heads, per)),
            dma((kv_heads, heads)),
            dma((pieces,)),
            dma((splits, kv_heads)),
            dma((kv_heads,)),
            dma((kv_heads,)),
        ],
        compiler_params=pltpu.CompilerParams(has_side_effects=True, vmem_limit_bytes=60 * 2**20),
        name="attention_grads",
    )(queries, key_head_matrix, value_head_matrix, attn_output, out_grad)


def solution(mesh):
    spec = P("span", "seq", None)
    return jax.shard_map(
        per_device, mesh=mesh, in_specs=(spec,) * 5, out_specs=(spec,) * 3, check_vma=False
    )
```

```python
import functools
import math

import jax
import jax.numpy as jnp
from jax import lax
from jax.experimental import pallas as pl
from jax.experimental.pallas import tpu as pltpu
from jax.sharding import PartitionSpec as P

HEAD_WIDTH = 64
PAIR = 2 * HEAD_WIDTH
QUERY_PER_KEY = 3
NEG_LARGE = -1e30
MESH = pl.DeviceIdType.MESH
LOG2E = math.log2(math.e)
SCORE_BYTES = 30 * 2**20


def dot(a, b, contract):
    return lax.dot_general(a, b, ((contract[:1], contract[1:]), ((), ())), preferred_element_type=jnp.float32)


def kernel(kv_heads, resident, q_ref, k_ref, v_ref, o_ref, g_ref, dq_in, dkv_in,
           qg_send, kv_send, dl_send, qg_in, kv_in, dl_in, q_pad, g_pad, dl_row, s_ref, m_ref, l_ref, dqt_ref,
           acc_ref, dq_send, mate_in, part_ref, red_in, fin_ref,
           qg_s, qg_r, kv_s, kv_r, dl_s, dl_r, side_s, hand_s, dq_s, dq_r, mate_s, mate_r, red_s, red_r, fin_s, fin_r):
    seq_count = lax.axis_size("seq")
    seq = lax.axis_index("seq")
    span = lax.axis_index("span")
    heads = QUERY_PER_KEY
    spread = lax.axis_size("span") // kv_heads
    splits = spread * seq_count
    tokens = q_ref.shape[1]
    per = kv_heads // 2
    chunk = per * tokens
    top = 2 * splits - 1
    me = span * seq_count + seq
    my_head = span // spread
    my_split = lax.rem(span, spread) * seq_count + seq
    scaling = 1.0 / math.sqrt(HEAD_WIDTH)
    factor = scaling * LOG2E

    def rank_of(split):
        return 2 * lax.rem(split, splits // 2) + split // (splits // 2)

    def split_of(rank):
        return lax.rem(rank, 2) * (splits // 2) + rank // 2

    my_rank = rank_of(my_split)
    my_chunk = me // per
    my_kind = jnp.where(my_chunk < splits, 0, 1)
    my_sub = lax.rem(me, per)
    q_split = split_of(jnp.where(my_chunk < splits, my_chunk, top - my_chunk))

    def far(a, t):
        turned, unit = 0, 1
        while unit < kv_heads:
            turned += lax.rem(a // unit + t // unit, 2) * unit
            unit *= 2
        return turned

    def chunk_of(kind):
        return top - my_rank if kind else my_rank

    def member(head, split):
        return {"seq": lax.rem(split, seq_count), "span": head * spread + split // seq_count}

    def source(piece):
        return {"seq": lax.rem(piece, seq_count), "span": piece // seq_count}

    def remote(src, dst, send, recv, device):
        return pltpu.make_async_remote_copy(src_ref=src, dst_ref=dst, send_sem=send, recv_sem=recv,
                                            device_id=device, device_id_type=MESH)

    def other(mine, fn_other, fn_mine):
        @pl.when(mine)
        def _():
            fn_mine()

        @pl.when(jnp.logical_not(mine))
        def _():
            fn_other()

    def qg_copy(h, j):
        return remote(qg_send.at[h, j], qg_in.at[my_kind, j, my_sub], qg_s.at[h, j], qg_r.at[my_kind, j, my_sub],
                      member(h, q_split))

    def qg_own(h, j):
        return pltpu.make_async_copy(qg_send.at[h, j], qg_in.at[my_kind, j, my_sub], qg_s.at[h, j])

    def dl_copy(h):
        return remote(dl_send.at[h], dl_in.at[my_kind, my_sub], dl_s.at[h], dl_r.at[my_kind, my_sub],
                      member(h, q_split))

    def dl_own(h):
        return pltpu.make_async_copy(dl_send.at[h], dl_in.at[my_kind, my_sub], dl_s.at[h])

    def q_mine(h):
        return jnp.logical_and(h == my_head, q_split == my_split)

    def kv_copy(h):
        return remote(kv_send.at[h], kv_in.at[me], kv_s.at[h], kv_r.at[me], member(h, my_split))

    def kv_own(h):
        return pltpu.make_async_copy(kv_send.at[h], kv_in.at[me], kv_s.at[h])

    twin = my_split + 1 - 2 * lax.rem(my_split, 2)

    def step_split(k):
        return lax.rem(my_split + 2 * k, splits)

    def hand_copy(i, k):
        piece = i * splits + my_split
        return remote(kv_in.at[piece], kv_in.at[piece], hand_s.at[k, i], kv_r.at[piece],
                      member(my_head, step_split(k)))

    def twin_copy(i, k):
        piece = i * splits + step_split(k)
        return remote(kv_in.at[piece], kv_in.at[piece], side_s.at[k, i], kv_r.at[piece], member(my_head, twin))

    def kv_wait(piece):
        remote(kv_in.at[piece], kv_in.at[piece], kv_s.at[0], kv_r.at[piece], member(my_head, twin)).wait_recv()

    def dq_copy(kind, j, sub):
        piece = chunk_of(kind) * per + sub
        return remote(dq_send.at[kind, j, sub], dq_in.at[my_head, j], dq_s.at[kind, j, sub], dq_r.at[my_head, j],
                      source(piece))

    def dq_own(kind, j, sub):
        return pltpu.make_async_copy(dq_send.at[kind, j, sub], dq_in.at[my_head, j], dq_s.at[kind, j, sub])

    def has(split, b):
        return top - rank_of(split) >= b

    side = lax.rem(my_split, 2)

    def mate_copy(b, u):
        at = pl.ds(pl.multiple_of((2 * u + 1 - side) * tokens, tokens), tokens)
        return remote(acc_ref.at[b, at, :], mate_in.at[b, u], mate_s.at[b, u], mate_r.at[b, u],
                      member(my_head, twin))

    def mate_wait(b, u):
        landing = mate_in.at[b, u]
        remote(landing, landing, mate_s.at[b, u], mate_r.at[b, u], member(my_head, twin)).wait_recv()

    def red_copy(piece):
        return remote(part_ref.at[piece], red_in.at[my_split // 2, piece // splits], red_s.at[piece],
                      red_r.at[my_split // 2, piece // splits], member(my_head, lax.rem(piece, splits)))

    def fin_copy(i):
        return remote(fin_ref.at[i], dkv_in.at[my_head], fin_s.at[i], fin_r.at[my_head],
                      source(i * splits + my_split))

    def fin_own(i):
        return pltpu.make_async_copy(fin_ref.at[i], dkv_in.at[my_head], fin_s.at[i])

    barrier = pltpu.get_barrier_semaphore()
    everyone = lax.axis_size("span") * seq_count

    def greet(d, _):
        @pl.when(d != me)
        def _():
            pl.semaphore_signal(barrier, inc=1, device_id=source(d), device_id_type=MESH)
        return 0

    lax.fori_loop(0, everyone, greet, 0)

    for h in range(kv_heads):
        at = slice(h * HEAD_WIDTH, (h + 1) * HEAD_WIDTH)
        kv_send[h] = jnp.concatenate([k_ref[0, :, at], v_ref[0, :, at]], axis=1)
    for h in range(kv_heads):
        for j in range(heads):
            one = h * heads + j
            at = slice(one * HEAD_WIDTH, (one + 1) * HEAD_WIDTH)
            qg_send[h, j] = jnp.concatenate([q_ref[0, :, at], g_ref[0, :, at]], axis=1)
    product = o_ref[0].astype(jnp.float32) * g_ref[0].astype(jnp.float32)
    high = product.astype(jnp.bfloat16)
    low = (product - high.astype(jnp.float32)).astype(jnp.bfloat16)
    wide = kv_heads * heads * HEAD_WIDTH
    row = lax.broadcasted_iota(jnp.int32, (kv_heads * 8, wide), 0)
    column = lax.broadcasted_iota(jnp.int32, (kv_heads * 8, wide), 1) // HEAD_WIDTH
    ones = jnp.where(row == (column // heads) * 8 + lax.rem(column, heads), 1.0, 0.0).astype(jnp.bfloat16)
    dl_send[...] = (dot(ones, high, (1, 1)) + dot(ones, low, (1, 1))).reshape(kv_heads, 8, tokens)

    def clear(b, _):
        acc_ref[b] = jnp.zeros((chunk, PAIR), jnp.float32)
        return 0

    lax.fori_loop(0, 2 * splits, clear, 0)
    pl.semaphore_wait(barrier, everyone - 1)

    def qg_start(j):
        for t in range(kv_heads):
            h = far(my_head, t)
            other(q_mine(h), lambda: qg_copy(h, j).start(), lambda: qg_own(h, j).start())

    for t in range(kv_heads):
        h = far(my_head, t)
        other(h == my_head, lambda: kv_copy(h).start(), lambda: kv_own(h).start())
    qg_start(0)
    for t in range(kv_heads):
        h = far(my_head, t)
        other(q_mine(h), lambda: dl_copy(h).start(), lambda: dl_own(h).start())

    def hand_on(t, _):
        i = far(my_head, t)
        piece = i * splits + my_split
        other(piece == me, lambda: kv_wait(piece), lambda: kv_own(my_head).wait())
        twin_copy(i, 0).start()
        for k in range(1, splits // 2):
            hand_copy(i, k).start()
        return 0

    lax.fori_loop(0, kv_heads, hand_on, 0)

    def pass_on(i, _):
        for k in range(1, splits // 2):
            kv_wait(i * splits + step_split(k))
            twin_copy(i, k).start()
        return 0

    lax.fori_loop(0, kv_heads, pass_on, 0)

    def twin_wait(i, _):
        for k in range(splits // 2):
            kv_wait(i * splits + lax.rem(twin + 2 * k, splits))
        return 0

    lax.fori_loop(0, kv_heads, twin_wait, 0)

    lane = lax.broadcasted_iota(jnp.int32, (1, PAIR), 1)

    def kv_block(b):
        return kv_in[pl.ds(b * per, per)].reshape(chunk, PAIR)

    def hide(s):
        k_pos = lax.broadcasted_iota(jnp.int32, (chunk, chunk), 0)
        q_pos = lax.broadcasted_iota(jnp.int32, (chunk, chunk), 1)
        return jnp.where(k_pos <= q_pos, s, NEG_LARGE)

    def scores(kind, b, j, last):
        s = dot(kv_block(b), q_pad[kind, j], (1, 1))
        return hide(s) if last else s

    def slot(kind, b):
        return (my_rank + 1) * kind + b

    def stats(kind, j):
        c_q = chunk_of(kind)
        for sub in range(per):
            mine = c_q * per + sub == me
            landing = qg_in.at[kind, j, sub]
            other(mine,
                  lambda: remote(landing, landing, qg_s.at[0, j], qg_r.at[kind, j, sub],
                                 member(my_head, twin)).wait_recv(),
                  lambda: qg_own(my_head, j).wait())
        both = qg_in[kind, j].reshape(chunk, PAIR)
        q_pad[kind, j] = jnp.where(lane < HEAD_WIDTH, both, jnp.zeros_like(both))
        g_pad[kind, j] = jnp.where(lane < HEAD_WIDTH, jnp.zeros_like(both), both)
        dqt_ref[kind, j] = jnp.zeros((HEAD_WIDTH, chunk), jnp.float32)
        m_ref[kind, j] = jnp.full((1, chunk), NEG_LARGE, jnp.float32)
        l_ref[kind, j] = jnp.zeros((1, chunk), jnp.float32)

        def block(b, last):
            s = scores(kind, b, j, last)
            if resident:
                s_ref[slot(kind, b)] = s
            m_old = m_ref[kind, j]
            m_new = jnp.maximum(m_old, jnp.max(s, axis=0, keepdims=True))
            e = jnp.exp2((s - m_new) * factor)
            l_ref[kind, j] = (l_ref[kind, j] * jnp.exp2((m_old - m_new) * factor)
                              + jnp.sum(e, axis=0, keepdims=True))
            m_ref[kind, j] = m_new
            return 0

        lax.fori_loop(0, c_q, lambda b, _: block(b, False), 0)
        block(c_q, True)
        m_ref[kind, j] = m_ref[kind, j] * factor + jnp.log2(l_ref[kind, j])

    def grads(kind, j, b, last):
        kv = kv_block(b)
        s = s_ref[slot(kind, b)] if resident else scores(kind, b, j, last)
        p = jnp.exp2(s * factor - m_ref[kind, j])
        dp = dot(kv, g_pad[kind, j], (1, 1))
        ds = (p * (dp - dl_row[kind, j])).astype(jnp.bfloat16)
        acc_ref[b] += dot(ds, q_pad[kind, j], (1, 0)) + dot(p.astype(jnp.bfloat16), g_pad[kind, j], (1, 0))
        dqt_ref[kind, j] += dot(kv[:, :HEAD_WIDTH].T, ds, (1, 0))

    def send_dq(kind, j):
        for sub in range(per):
            part = dqt_ref[kind, j, :, sub * tokens:(sub + 1) * tokens] * scaling
            dq_send[kind, j, sub] = part.astype(jnp.bfloat16)
        for sub in range(per):
            other(chunk_of(kind) * per + sub == me, lambda: dq_copy(kind, j, sub).start(),
                  lambda: dq_own(kind, j, sub).start())

    def job(kind, j):
        c_q = chunk_of(kind)
        lax.fori_loop(0, c_q, lambda b, _: (grads(kind, j, b, False), 0)[1], 0)
        grads(kind, j, c_q, True)
        send_dq(kind, j)

    weight = jnp.where(lane < HEAD_WIDTH, scaling, 1.0)

    def own_piece(b, u):
        return b * per + 2 * u + side

    def own_rows(u):
        return pl.ds(pl.multiple_of((2 * u + side) * tokens, tokens), tokens)

    def pair_sends(b, u):
        return jnp.logical_and(lax.rem(own_piece(b, u), splits) != my_split,
                               jnp.logical_or(has(my_split, b), has(twin, b)))

    def hand_out(b):
        for u in range(per // 2):
            mate_copy(b, u).start()

    def pair_sum(b):
        @pl.when(has(twin, b))
        def _():
            for u in range(per // 2):
                mate_wait(b, u)
                acc_ref[b, own_rows(u), :] += mate_in[b, u]

        for u in range(per // 2):
            @pl.when(pair_sends(b, u))
            def _():
                piece = own_piece(b, u)
                part_ref[piece] = (acc_ref[b, own_rows(u), :] * weight).astype(jnp.bfloat16)
                red_copy(piece).start()

    def reduce(b):
        for u in range(per // 2):
            piece = own_piece(b, u)

            @pl.when(lax.rem(piece, splits) == my_split)
            def _():
                i = piece // splits
                total = acc_ref.at[b, own_rows(u), :]
                total[...] = total[...] * weight

                def add(f, _):
                    @pl.when(jnp.logical_and(f != my_split // 2,
                                             jnp.logical_or(has(2 * f, b), has(2 * f + 1, b))))
                    def _():
                        landing = red_in.at[f, i]
                        remote(landing, landing, red_s.at[0], red_r.at[f, i], member(my_head, twin)).wait_recv()
                        total[...] += red_in[f, i].astype(jnp.float32)
                    return 0

                lax.fori_loop(0, splits // 2, add, 0)
                fin_ref[i] = total[...].astype(jnp.bfloat16)
                other(piece == me, lambda: fin_copy(i).start(), lambda: fin_own(i).start())

    for kind in range(2):
        c_q = chunk_of(kind)
        for sub in range(per):
            small = dl_in.at[kind, sub]
            other(c_q * per + sub == me,
                  lambda: remote(small, small, dl_s.at[0], dl_r.at[kind, sub], member(my_head, twin)).wait_recv(),
                  lambda: dl_own(my_head).wait())
        for j in range(heads):
            for sub in range(per):
                dl_row[kind, j, :, sub * tokens:(sub + 1) * tokens] = dl_in[kind, sub, pl.ds(j, 1), :]

    def whole_head(j, _):
        stats(0, j)
        qg_start(j + 1)
        stats(1, j)
        for kind in range(2):
            job(kind, j)
        return 0

    lax.fori_loop(0, heads - 1, whole_head, 0)
    final = heads - 1
    for kind in range(2):
        stats(kind, final)
    job(0, final)

    def sweep(t, _):
        b = top - t

        @pl.when(b < chunk_of(1))
        def _():
            grads(1, final, b, False)

        @pl.when(b == chunk_of(1))
        def _():
            grads(1, final, b, True)

        @pl.when(b <= chunk_of(1))
        def _():
            hand_out(b)

        @pl.when(t > 0)
        def _():
            pair_sum(b + 1)

        @pl.when(t > 1)
        def _():
            reduce(b + 2)
        return 0

    lax.fori_loop(0, top + 1, sweep, 0)
    send_dq(1, final)
    pair_sum(0)
    reduce(1)
    reduce(0)

    for h in range(kv_heads):
        for j in range(heads):
            mine = q_mine(h)
            landing = dq_in.at[h, j]
            other(mine,
                  lambda: remote(landing, landing, dq_s.at[0, j, 0], dq_r.at[h, j], member(my_head, twin)).wait_recv(),
                  lambda: dq_own(my_kind, j, my_sub).wait())
    for h in range(kv_heads):
        landing = dkv_in.at[h]
        other(h == my_head,
              lambda: remote(landing, landing, fin_s.at[0], fin_r.at[h], member(my_head, twin)).wait_recv(),
              lambda: fin_own(my_head).wait())
    for h in range(kv_heads):
        @pl.when(h != my_head)
        def _():
            kv_copy(h).wait_send()

        @pl.when(jnp.logical_not(q_mine(h)))
        def _():
            dl_copy(h).wait_send()
            for j in range(heads):
                qg_copy(h, j).wait_send()

    def sent(i, _):
        for k in range(splits // 2):
            twin_copy(i, k).wait_send()
            if k:
                hand_copy(i, k).wait_send()

        @pl.when(i != my_head)
        def _():
            fin_copy(i).wait_send()
        return 0

    lax.fori_loop(0, kv_heads, sent, 0)
    for kind in range(2):
        for j in range(heads):
            for sub in range(per):
                @pl.when(chunk_of(kind) * per + sub != me)
                def _():
                    dq_copy(kind, j, sub).wait_send()

    def red_sent(b, _):
        for u in range(per // 2):
            @pl.when(has(my_split, b))
            def _():
                mate_copy(b, u).wait_send()

            @pl.when(pair_sends(b, u))
            def _():
                red_copy(own_piece(b, u)).wait_send()
        return 0

    lax.fori_loop(0, top + 1, red_sent, 0)


def results(dq_in, dkv_in, dq_out, dk_out, dv_out):
    kv_heads, heads, _, tokens = dq_in.shape
    dq_out[0] = dq_in[...].reshape(kv_heads * heads * HEAD_WIDTH, tokens).T
    for h in range(0, kv_heads, 2):
        at = slice(h * HEAD_WIDTH, (h + 2) * HEAD_WIDTH)
        dk_out[0, :, at] = jnp.concatenate([dkv_in[h, :, :HEAD_WIDTH], dkv_in[h + 1, :, :HEAD_WIDTH]], axis=1)
        dv_out[0, :, at] = jnp.concatenate([dkv_in[h, :, HEAD_WIDTH:], dkv_in[h + 1, :, HEAD_WIDTH:]], axis=1)


def vmem(count):
    return [pl.BlockSpec(memory_space=pltpu.VMEM)] * count


def per_device(queries, key_head_matrix, value_head_matrix, attn_output, out_grad):
    seq_count = lax.axis_size("seq")
    tokens = queries.shape[1]
    kv_heads = key_head_matrix.shape[2] // HEAD_WIDTH
    splits = lax.axis_size("span") // kv_heads * seq_count
    pieces = kv_heads * splits
    heads = QUERY_PER_KEY
    per = kv_heads // 2
    chunk = per * tokens
    count = 2 * splits + 1
    resident = count * chunk * chunk * 4 <= SCORE_BYTES
    dma = pltpu.SemaphoreType.DMA
    low, full = jnp.bfloat16, jnp.float32
    dq, dkv = pl.pallas_call(
        functools.partial(kernel, kv_heads, resident),
        out_shape=(
            jax.ShapeDtypeStruct((kv_heads, heads, HEAD_WIDTH, tokens), low),
            jax.ShapeDtypeStruct((kv_heads, tokens, PAIR), low),
        ),
        in_specs=vmem(5),
        out_specs=tuple(vmem(2)),
        scratch_shapes=[
            pltpu.VMEM((kv_heads, heads, tokens, PAIR), low),
            pltpu.VMEM((kv_heads, tokens, PAIR), low),
            pltpu.VMEM((kv_heads, 8, tokens), full),
            pltpu.VMEM((2, heads, per, tokens, PAIR), low),
            pltpu.VMEM((pieces, tokens, PAIR), low),
            pltpu.VMEM((2, per, 8, tokens), full),
            pltpu.VMEM((2, heads, chunk, PAIR), low),
            pltpu.VMEM((2, heads, chunk, PAIR), low),
            pltpu.VMEM((2, heads, 1, chunk), full),
            pltpu.VMEM((count, chunk, chunk) if resident else (1, 8, chunk), full),
            pltpu.VMEM((2, heads, 1, chunk), full),
            pltpu.VMEM((2, heads, 1, chunk), full),
            pltpu.VMEM((2, heads, HEAD_WIDTH, chunk), full),
            pltpu.VMEM((2 * splits, chunk, PAIR), full),
            pltpu.VMEM((2, heads, per, HEAD_WIDTH, tokens), low),
            pltpu.VMEM((2 * splits, per // 2, tokens, PAIR), full),
            pltpu.VMEM((pieces, tokens, PAIR), low),
            pltpu.VMEM((splits // 2, kv_heads, tokens, PAIR), low),
            pltpu.VMEM((kv_heads, tokens, PAIR), low),
            dma((kv_heads, heads)),
            dma((2, heads, per)),
            dma((kv_heads,)),
            dma((pieces,)),
            dma((kv_heads,)),
            dma((2, per)),
            dma((splits // 2, kv_heads)),
            dma((splits // 2, kv_heads)),
            dma((2, heads, per)),
            dma((kv_heads, heads)),
            dma((2 * splits, per // 2)),
            dma((2 * splits, per // 2)),
            dma((pieces,)),
            dma((splits // 2, kv_heads)),
            dma((kv_heads,)),
            dma((kv_heads,)),
        ],
        compiler_params=pltpu.CompilerParams(collective_id=0, has_side_effects=True, vmem_limit_bytes=60 * 2**20),
        name="attention_grads",
    )(queries, key_head_matrix, value_head_matrix, attn_output, out_grad)
    return pl.pallas_call(
        results,
        out_shape=(
            jax.ShapeDtypeStruct(queries.shape, low),
            jax.ShapeDtypeStruct(key_head_matrix.shape, low),
            jax.ShapeDtypeStruct(value_head_matrix.shape, low),
        ),
        in_specs=vmem(2),
        out_specs=tuple(vmem(3)),
        name="results",
    )(dq, dkv)


def solution(mesh):
    spec = P("span", "seq", None)
    return jax.shard_map(
        per_device, mesh=mesh, in_specs=(spec,) * 5, out_specs=(spec,) * 3, check_vma=False
    )
```

```python
import functools
import math

import jax
import jax.numpy as jnp
from jax import lax
from jax.experimental import pallas as pl
from jax.experimental.pallas import tpu as pltpu
from jax.sharding import PartitionSpec as P

HEAD_WIDTH = 64
PAIR = 2 * HEAD_WIDTH
QUERY_PER_KEY = 3
NEG_LARGE = -1e30
MESH = pl.DeviceIdType.MESH
LOG2E = math.log2(math.e)
SCORE_BYTES = 30 * 2**20
SUM_LAG = 2
REDUCE_LAG = 5


def dot(a, b, contract):
    return lax.dot_general(a, b, ((contract[:1], contract[1:]), ((), ())), preferred_element_type=jnp.float32)


def kernel(kv_heads, resident, q_ref, k_ref, v_ref, o_ref, g_ref, dq_in, dkv_in,
           qg_send, kv_send, dl_send, qg_in, kv_in, dl_in, q_pad, g_pad, dl_row, s0_ref, s1_ref, p0_ref, p1_ref, ds0_ref, ds1_ref, m_ref, dqt_ref,
           acc_ref, dq_send, mate_in, part_ref, red_in, fin_ref,
           qg_s, qg_r, kv_s, kv_r, dl_s, dl_r, side_s, hand_s, dq_s, dq_r, mate_s, mate_r, red_s, red_r, fin_s, fin_r):
    seq_count = lax.axis_size("seq")
    seq = lax.axis_index("seq")
    span = lax.axis_index("span")
    heads = QUERY_PER_KEY
    spread = lax.axis_size("span") // kv_heads
    splits = spread * seq_count
    tokens = q_ref.shape[1]
    per = kv_heads // 2
    chunk = per * tokens
    top = 2 * splits - 1
    me = span * seq_count + seq
    my_head = span // spread
    my_split = lax.rem(span, spread) * seq_count + seq
    scaling = 1.0 / math.sqrt(HEAD_WIDTH)
    factor = scaling * LOG2E

    def rank_of(split):
        return 2 * lax.rem(split, splits // 2) + split // (splits // 2)

    def split_of(rank):
        return lax.rem(rank, 2) * (splits // 2) + rank // 2

    my_rank = rank_of(my_split)
    my_chunk = me // per
    my_kind = jnp.where(my_chunk < splits, 0, 1)
    my_sub = lax.rem(me, per)
    q_split = split_of(jnp.where(my_chunk < splits, my_chunk, top - my_chunk))

    def far(a, t):
        turned, unit = 0, 1
        while unit < kv_heads:
            turned += lax.rem(a // unit + t // unit, 2) * unit
            unit *= 2
        return turned

    def chunk_of(kind):
        return top - my_rank if kind else my_rank

    def member(head, split):
        return {"seq": lax.rem(split, seq_count), "span": head * spread + split // seq_count}

    def source(piece):
        return {"seq": lax.rem(piece, seq_count), "span": piece // seq_count}

    def remote(src, dst, send, recv, device):
        return pltpu.make_async_remote_copy(src_ref=src, dst_ref=dst, send_sem=send, recv_sem=recv,
                                            device_id=device, device_id_type=MESH)

    def other(mine, fn_other, fn_mine):
        @pl.when(mine)
        def _():
            fn_mine()

        @pl.when(jnp.logical_not(mine))
        def _():
            fn_other()

    def qg_copy(h, j):
        return remote(qg_send.at[h, j], qg_in.at[my_kind, j, my_sub], qg_s.at[h, j], qg_r.at[my_kind, j, my_sub],
                      member(h, q_split))

    def qg_own(h, j):
        return pltpu.make_async_copy(qg_send.at[h, j], qg_in.at[my_kind, j, my_sub], qg_s.at[h, j])

    def dl_copy(h):
        return remote(dl_send.at[h], dl_in.at[my_kind, my_sub], dl_s.at[h], dl_r.at[my_kind, my_sub],
                      member(h, q_split))

    def dl_own(h):
        return pltpu.make_async_copy(dl_send.at[h], dl_in.at[my_kind, my_sub], dl_s.at[h])

    def q_mine(h):
        return jnp.logical_and(h == my_head, q_split == my_split)

    def kv_copy(h):
        return remote(kv_send.at[h], kv_in.at[me], kv_s.at[h], kv_r.at[me], member(h, my_split))

    def kv_own(h):
        return pltpu.make_async_copy(kv_send.at[h], kv_in.at[me], kv_s.at[h])

    twin = my_split + 1 - 2 * lax.rem(my_split, 2)

    def step_split(k):
        return lax.rem(my_split + 2 * k, splits)

    def hand_copy(i, k):
        piece = i * splits + my_split
        return remote(kv_in.at[piece], kv_in.at[piece], hand_s.at[k, i], kv_r.at[piece],
                      member(my_head, step_split(k)))

    def twin_copy(i, k):
        piece = i * splits + step_split(k)
        return remote(kv_in.at[piece], kv_in.at[piece], side_s.at[k, i], kv_r.at[piece], member(my_head, twin))

    def kv_wait(piece):
        remote(kv_in.at[piece], kv_in.at[piece], kv_s.at[0], kv_r.at[piece], member(my_head, twin)).wait_recv()

    def dq_copy(kind, j, sub):
        piece = chunk_of(kind) * per + sub
        return remote(dq_send.at[kind, j, sub], dq_in.at[my_head, j], dq_s.at[kind, j, sub], dq_r.at[my_head, j],
                      source(piece))

    def dq_own(kind, j, sub):
        return pltpu.make_async_copy(dq_send.at[kind, j, sub], dq_in.at[my_head, j], dq_s.at[kind, j, sub])

    def has(split, b):
        return top - rank_of(split) >= b

    side = lax.rem(my_split, 2)

    def mate_copy(b, u):
        at = pl.ds(pl.multiple_of((2 * u + 1 - side) * tokens, tokens), tokens)
        return remote(acc_ref.at[b, at, :], mate_in.at[b, u], mate_s.at[b, u], mate_r.at[b, u],
                      member(my_head, twin))

    def mate_wait(b, u):
        landing = mate_in.at[b, u]
        remote(landing, landing, mate_s.at[b, u], mate_r.at[b, u], member(my_head, twin)).wait_recv()

    def red_copy(piece):
        return remote(part_ref.at[piece], red_in.at[my_split // 2, piece // splits], red_s.at[piece],
                      red_r.at[my_split // 2, piece // splits], member(my_head, lax.rem(piece, splits)))

    def fin_copy(i):
        return remote(fin_ref.at[i], dkv_in.at[my_head], fin_s.at[i], fin_r.at[my_head],
                      source(i * splits + my_split))

    def fin_own(i):
        return pltpu.make_async_copy(fin_ref.at[i], dkv_in.at[my_head], fin_s.at[i])

    barrier = pltpu.get_barrier_semaphore()
    everyone = lax.axis_size("span") * seq_count

    def greet(d, _):
        @pl.when(d != me)
        def _():
            pl.semaphore_signal(barrier, inc=1, device_id=source(d), device_id_type=MESH)
        return 0

    lax.fori_loop(0, everyone, greet, 0)

    for h in range(kv_heads):
        at = slice(h * HEAD_WIDTH, (h + 1) * HEAD_WIDTH)
        kv_send[h] = jnp.concatenate([k_ref[0, :, at], v_ref[0, :, at]], axis=1)
    for h in range(kv_heads):
        for j in range(heads):
            one = h * heads + j
            at = slice(one * HEAD_WIDTH, (one + 1) * HEAD_WIDTH)
            qg_send[h, j] = jnp.concatenate([q_ref[0, :, at], g_ref[0, :, at]], axis=1)
    product = o_ref[0].astype(jnp.float32) * g_ref[0].astype(jnp.float32)
    high = product.astype(jnp.bfloat16)
    low = (product - high.astype(jnp.float32)).astype(jnp.bfloat16)
    wide = kv_heads * heads * HEAD_WIDTH
    row = lax.broadcasted_iota(jnp.int32, (kv_heads * 8, wide), 0)
    column = lax.broadcasted_iota(jnp.int32, (kv_heads * 8, wide), 1) // HEAD_WIDTH
    ones = jnp.where(row == (column // heads) * 8 + lax.rem(column, heads), 1.0, 0.0).astype(jnp.bfloat16)
    dl_send[...] = (dot(ones, high, (1, 1)) + dot(ones, low, (1, 1))).reshape(kv_heads, 8, tokens)

    def clear(b, _):
        acc_ref[b] = jnp.zeros((chunk, PAIR), jnp.float32)
        return 0

    lax.fori_loop(0, 2 * splits, clear, 0)
    pl.semaphore_wait(barrier, everyone - 1)

    def qg_start(j):
        for t in range(kv_heads):
            h = far(my_head, t)
            other(q_mine(h), lambda: qg_copy(h, j).start(), lambda: qg_own(h, j).start())

    for t in range(kv_heads):
        h = far(my_head, t)
        other(h == my_head, lambda: kv_copy(h).start(), lambda: kv_own(h).start())
    qg_start(0)
    for t in range(kv_heads):
        h = far(my_head, t)
        other(q_mine(h), lambda: dl_copy(h).start(), lambda: dl_own(h).start())

    def hand_on(t, _):
        i = far(my_head, t)
        piece = i * splits + my_split
        other(piece == me, lambda: kv_wait(piece), lambda: kv_own(my_head).wait())
        twin_copy(i, 0).start()
        for k in range(1, splits // 2):
            hand_copy(i, k).start()
        return 0

    lax.fori_loop(0, kv_heads, hand_on, 0)

    def pass_on(i, _):
        for k in range(1, splits // 2):
            kv_wait(i * splits + step_split(k))
            twin_copy(i, k).start()
        return 0

    lax.fori_loop(0, kv_heads, pass_on, 0)

    def twin_wait(i, _):
        for k in range(splits // 2):
            kv_wait(i * splits + lax.rem(twin + 2 * k, splits))
        return 0

    lax.fori_loop(0, kv_heads, twin_wait, 0)

    lane = lax.broadcasted_iota(jnp.int32, (1, PAIR), 1)

    half = chunk // 2
    s_refs = (s0_ref, s1_ref)
    p_refs = (p0_ref, p1_ref)
    ds_refs = (ds0_ref, ds1_ref)

    def kv_half(b, side_of):
        return kv_in[pl.ds(b * per + side_of * (per // 2), per // 2)].reshape(half, PAIR)

    def hide(s, side_of):
        k_pos = side_of * half + lax.broadcasted_iota(jnp.int32, (half, chunk), 0)
        q_pos = lax.broadcasted_iota(jnp.int32, (half, chunk), 1)
        return jnp.where(k_pos <= q_pos, s, NEG_LARGE)

    def scores(kind, j, b, side_of):
        return dot(kv_half(b, side_of), q_pad[kind, j], (1, 1))

    def top_of(s):
        return jnp.max(s, axis=0, keepdims=True)

    def slot(kind, b):
        return (my_rank + 1) * kind + b if resident else 0

    def stats(kind, j):
        c_q = chunk_of(kind)
        for sub in range(per):
            mine = c_q * per + sub == me
            landing = qg_in.at[kind, j, sub]
            other(mine,
                  lambda: remote(landing, landing, qg_s.at[0, j], qg_r.at[kind, j, sub],
                                 member(my_head, twin)).wait_recv(),
                  lambda: qg_own(my_head, j).wait())
        both = qg_in[kind, j].reshape(chunk, PAIR)
        q_pad[kind, j] = jnp.where(lane < HEAD_WIDTH, both, jnp.zeros_like(both))
        g_pad[kind, j] = jnp.where(lane < HEAD_WIDTH, jnp.zeros_like(both), both)
        dqt_ref[kind, j] = jnp.zeros((HEAD_WIDTH, chunk), jnp.float32)

        def make(b, side_of):
            s = scores(kind, j, b, side_of)
            s_refs[side_of][slot(kind, b)] = s
            return top_of(s)

        def take(b, side_of, seen, m_old, l_old):
            m_new = jnp.maximum(m_old, seen)
            e = jnp.exp2((s_refs[side_of][slot(kind, b)] - m_new) * factor)
            l_new = l_old * jnp.exp2((m_old - m_new) * factor) + jnp.sum(e, axis=0, keepdims=True)
            return m_new, l_new

        def block(b, carry):
            seen, m, l = carry
            later = make(b, 1)
            m, l = take(b, 0, seen, m, l)
            following = make(b + 1, 0)
            m, l = take(b, 1, later, m, l)
            return following, m, l

        start = (make(0, 0), jnp.full((1, chunk), NEG_LARGE, jnp.float32), jnp.zeros((1, chunk), jnp.float32))
        _, m, l = lax.fori_loop(0, c_q, block, start)
        make(c_q, 1)
        for side_of in range(2):
            s = hide(s_refs[side_of][slot(kind, c_q)], side_of)
            s_refs[side_of][slot(kind, c_q)] = s
            m, l = take(c_q, side_of, top_of(s), m, l)
        m_ref[kind, j] = m * factor + jnp.log2(l)

    def weigh(kind, j, b, side_of):
        kv = kv_half(b, side_of)
        if resident:
            s = s_refs[side_of][slot(kind, b)]
        else:
            s = scores(kind, j, b, side_of)
            k_pos = b * chunk + side_of * half + lax.broadcasted_iota(jnp.int32, (half, chunk), 0)
            q_pos = chunk_of(kind) * chunk + lax.broadcasted_iota(jnp.int32, (half, chunk), 1)
            s = jnp.where(k_pos <= q_pos, s, NEG_LARGE)
        p = jnp.exp2(s * factor - m_ref[kind, j])
        dp = dot(kv, g_pad[kind, j], (1, 1))
        ds_refs[side_of][...] = (p * (dp - dl_row[kind, j])).astype(jnp.bfloat16)
        p_refs[side_of][...] = p.astype(jnp.bfloat16)

    def gather(kind, j, b, side_of):
        ds = ds_refs[side_of][...]
        at = pl.ds(side_of * half, half)
        acc_ref[b, at, :] += dot(ds, q_pad[kind, j], (1, 0)) + dot(p_refs[side_of][...], g_pad[kind, j], (1, 0))
        dqt_ref[kind, j] += dot(kv_half(b, side_of)[:, :HEAD_WIDTH].T, ds, (1, 0))

    def open_job(kind, j, b):
        weigh(kind, j, b, 0)
        weigh(kind, j, b, 1)
        gather(kind, j, b, 0)

    def next_block(kind, j, before, b):
        weigh(kind, j, b, 0)
        gather(kind, j, before, 1)
        weigh(kind, j, b, 1)
        gather(kind, j, b, 0)

    def send_dq(kind, j):
        for sub in range(per):
            part = dqt_ref[kind, j, :, sub * tokens:(sub + 1) * tokens] * scaling
            dq_send[kind, j, sub] = part.astype(jnp.bfloat16)
        for sub in range(per):
            other(chunk_of(kind) * per + sub == me, lambda: dq_copy(kind, j, sub).start(),
                  lambda: dq_own(kind, j, sub).start())

    def job(kind, j):
        c_q = chunk_of(kind)
        open_job(kind, j, 0)
        lax.fori_loop(1, c_q + 1, lambda b, _: (next_block(kind, j, b - 1, b), 0)[1], 0)
        gather(kind, j, c_q, 1)
        send_dq(kind, j)

    weight = jnp.where(lane < HEAD_WIDTH, scaling, 1.0)

    def own_piece(b, u):
        return b * per + 2 * u + side

    def own_rows(u):
        return pl.ds(pl.multiple_of((2 * u + side) * tokens, tokens), tokens)

    def pair_sends(b, u):
        return jnp.logical_and(lax.rem(own_piece(b, u), splits) != my_split,
                               jnp.logical_or(has(my_split, b), has(twin, b)))

    def hand_out(b):
        for u in range(per // 2):
            mate_copy(b, u).start()

    def pair_sum(b):
        @pl.when(has(twin, b))
        def _():
            for u in range(per // 2):
                mate_wait(b, u)
                acc_ref[b, own_rows(u), :] += mate_in[b, u]

        for u in range(per // 2):
            @pl.when(pair_sends(b, u))
            def _():
                piece = own_piece(b, u)
                part_ref[piece] = (acc_ref[b, own_rows(u), :] * weight).astype(jnp.bfloat16)
                red_copy(piece).start()

    def reduce(b):
        for u in range(per // 2):
            piece = own_piece(b, u)

            @pl.when(lax.rem(piece, splits) == my_split)
            def _():
                i = piece // splits
                total = acc_ref.at[b, own_rows(u), :]
                total[...] = total[...] * weight

                def add(f, _):
                    @pl.when(jnp.logical_and(f != my_split // 2,
                                             jnp.logical_or(has(2 * f, b), has(2 * f + 1, b))))
                    def _():
                        landing = red_in.at[f, i]
                        remote(landing, landing, red_s.at[0], red_r.at[f, i], member(my_head, twin)).wait_recv()
                        total[...] += red_in[f, i].astype(jnp.float32)
                    return 0

                lax.fori_loop(0, splits // 2, add, 0)
                fin_ref[i] = total[...].astype(jnp.bfloat16)
                other(piece == me, lambda: fin_copy(i).start(), lambda: fin_own(i).start())

    for kind in range(2):
        c_q = chunk_of(kind)
        for sub in range(per):
            small = dl_in.at[kind, sub]
            other(c_q * per + sub == me,
                  lambda: remote(small, small, dl_s.at[0], dl_r.at[kind, sub], member(my_head, twin)).wait_recv(),
                  lambda: dl_own(my_head).wait())
        for j in range(heads):
            for sub in range(per):
                dl_row[kind, j, :, sub * tokens:(sub + 1) * tokens] = dl_in[kind, sub, pl.ds(j, 1), :]

    def whole_head(j, _):
        stats(0, j)
        qg_start(j + 1)
        stats(1, j)
        for kind in range(2):
            job(kind, j)
        return 0

    lax.fori_loop(0, heads - 1, whole_head, 0)
    final = heads - 1
    for kind in range(2):
        stats(kind, final)
    job(0, final)

    def turn(t):
        return jnp.where(t < splits, top - t, lax.rem(t + my_head, splits))

    def tidy(t, _):
        @pl.when(t >= SUM_LAG)
        def _():
            pair_sum(turn(t - SUM_LAG))

        @pl.when(t >= REDUCE_LAG)
        def _():
            reduce(turn(t - REDUCE_LAG))
        return 0

    def sweep(t, _):
        next_block(1, final, turn(t - 1), turn(t))
        hand_out(turn(t - 1))
        return tidy(t, 0)

    def late_sum(t, _):
        pair_sum(turn(t))
        return 0

    def late_reduce(t, _):
        reduce(turn(t))
        return 0

    lax.fori_loop(0, my_rank + 1, tidy, 0)
    open_job(1, final, chunk_of(1))
    lax.fori_loop(my_rank + 1, top + 1, sweep, 0)
    gather(1, final, turn(top), 1)
    hand_out(turn(top))
    send_dq(1, final)
    middle = top + 1 - SUM_LAG
    start = max(0, top + 1 - REDUCE_LAG)
    lax.fori_loop(start, middle, late_reduce, 0)
    lax.fori_loop(middle, top + 1, late_sum, 0)
    lax.fori_loop(middle, top + 1, late_reduce, 0)

    for h in range(kv_heads):
        @pl.when(h != my_head)
        def _():
            kv_copy(h).wait_send()

        @pl.when(jnp.logical_not(q_mine(h)))
        def _():
            dl_copy(h).wait_send()
            for j in range(heads):
                qg_copy(h, j).wait_send()

    def sent(i, _):
        for k in range(splits // 2):
            twin_copy(i, k).wait_send()
            if k:
                hand_copy(i, k).wait_send()

        @pl.when(i != my_head)
        def _():
            fin_copy(i).wait_send()
        return 0

    lax.fori_loop(0, kv_heads, sent, 0)
    for kind in range(2):
        for j in range(heads):
            for sub in range(per):
                @pl.when(chunk_of(kind) * per + sub != me)
                def _():
                    dq_copy(kind, j, sub).wait_send()

    def red_sent(b, _):
        for u in range(per // 2):
            @pl.when(has(my_split, b))
            def _():
                mate_copy(b, u).wait_send()

            @pl.when(pair_sends(b, u))
            def _():
                red_copy(own_piece(b, u)).wait_send()
        return 0

    lax.fori_loop(0, top + 1, red_sent, 0)

    for h in range(kv_heads):
        for j in range(heads):
            mine = q_mine(h)
            landing = dq_in.at[h, j]
            other(mine,
                  lambda: remote(landing, landing, dq_s.at[0, j, 0], dq_r.at[h, j], member(my_head, twin)).wait_recv(),
                  lambda: dq_own(my_kind, j, my_sub).wait())
    for h in range(kv_heads):
        landing = dkv_in.at[h]
        other(h == my_head,
              lambda: remote(landing, landing, fin_s.at[0], fin_r.at[h], member(my_head, twin)).wait_recv(),
              lambda: fin_own(my_head).wait())


def results(dq_in, dkv_in, dq_out, dk_out, dv_out):
    kv_heads, heads, _, tokens = dq_in.shape
    dq_out[0] = dq_in[...].reshape(kv_heads * heads * HEAD_WIDTH, tokens).T
    for h in range(0, kv_heads, 2):
        at = slice(h * HEAD_WIDTH, (h + 2) * HEAD_WIDTH)
        dk_out[0, :, at] = jnp.concatenate([dkv_in[h, :, :HEAD_WIDTH], dkv_in[h + 1, :, :HEAD_WIDTH]], axis=1)
        dv_out[0, :, at] = jnp.concatenate([dkv_in[h, :, HEAD_WIDTH:], dkv_in[h + 1, :, HEAD_WIDTH:]], axis=1)


def vmem(count):
    return [pl.BlockSpec(memory_space=pltpu.VMEM)] * count


def per_device(queries, key_head_matrix, value_head_matrix, attn_output, out_grad):
    seq_count = lax.axis_size("seq")
    tokens = queries.shape[1]
    kv_heads = key_head_matrix.shape[2] // HEAD_WIDTH
    splits = lax.axis_size("span") // kv_heads * seq_count
    pieces = kv_heads * splits
    heads = QUERY_PER_KEY
    per = kv_heads // 2
    chunk = per * tokens
    count = 2 * splits + 1
    resident = count * chunk * chunk * 4 <= SCORE_BYTES
    count = count if resident else 1
    dma = pltpu.SemaphoreType.DMA
    low, full = jnp.bfloat16, jnp.float32
    dq, dkv = pl.pallas_call(
        functools.partial(kernel, kv_heads, resident),
        out_shape=(
            jax.ShapeDtypeStruct((kv_heads, heads, HEAD_WIDTH, tokens), low),
            jax.ShapeDtypeStruct((kv_heads, tokens, PAIR), low),
        ),
        in_specs=vmem(5),
        out_specs=tuple(vmem(2)),
        scratch_shapes=[
            pltpu.VMEM((kv_heads, heads, tokens, PAIR), low),
            pltpu.VMEM((kv_heads, tokens, PAIR), low),
            pltpu.VMEM((kv_heads, 8, tokens), full),
            pltpu.VMEM((2, heads, per, tokens, PAIR), low),
            pltpu.VMEM((pieces, tokens, PAIR), low),
            pltpu.VMEM((2, per, 8, tokens), full),
            pltpu.VMEM((2, heads, chunk, PAIR), low),
            pltpu.VMEM((2, heads, chunk, PAIR), low),
            pltpu.VMEM((2, heads, 1, chunk), full),
            pltpu.VMEM((count, chunk // 2, chunk), full),
            pltpu.VMEM((count, chunk // 2, chunk), full),
            pltpu.VMEM((chunk // 2, chunk), low),
            pltpu.VMEM((chunk // 2, chunk), low),
            pltpu.VMEM((chunk // 2, chunk), low),
            pltpu.VMEM((chunk // 2, chunk), low),
            pltpu.VMEM((2, heads, 1, chunk), full),
            pltpu.VMEM((2, heads, HEAD_WIDTH, chunk), full),
            pltpu.VMEM((2 * splits, chunk, PAIR), full),
            pltpu.VMEM((2, heads, per, HEAD_WIDTH, tokens), low),
            pltpu.VMEM((2 * splits, per // 2, tokens, PAIR), full),
            pltpu.VMEM((pieces, tokens, PAIR), low),
            pltpu.VMEM((splits // 2, kv_heads, tokens, PAIR), low),
            pltpu.VMEM((kv_heads, tokens, PAIR), low),
            dma((kv_heads, heads)),
            dma((2, heads, per)),
            dma((kv_heads,)),
            dma((pieces,)),
            dma((kv_heads,)),
            dma((2, per)),
            dma((splits // 2, kv_heads)),
            dma((splits // 2, kv_heads)),
            dma((2, heads, per)),
            dma((kv_heads, heads)),
            dma((2 * splits, per // 2)),
            dma((2 * splits, per // 2)),
            dma((pieces,)),
            dma((splits // 2, kv_heads)),
            dma((kv_heads,)),
            dma((kv_heads,)),
        ],
        compiler_params=pltpu.CompilerParams(collective_id=0, has_side_effects=True, vmem_limit_bytes=60 * 2**20),
        name="attention_grads",
    )(queries, key_head_matrix, value_head_matrix, attn_output, out_grad)
    return pl.pallas_call(
        results,
        out_shape=(
            jax.ShapeDtypeStruct(queries.shape, low),
            jax.ShapeDtypeStruct(key_head_matrix.shape, low),
            jax.ShapeDtypeStruct(value_head_matrix.shape, low),
        ),
        in_specs=vmem(2),
        out_specs=tuple(vmem(3)),
        name="results",
    )(dq, dkv)


def solution(mesh):
    spec = P("span", "seq", None)
    return jax.shard_map(
        per_device, mesh=mesh, in_specs=(spec,) * 5, out_specs=(spec,) * 3, check_vma=False
    )
```

```python
import functools
import math

import jax
import jax.numpy as jnp
from jax import lax
from jax.experimental import pallas as pl
from jax.experimental.pallas import tpu as pltpu
from jax.sharding import PartitionSpec as P

HEAD_WIDTH = 64
PAIR = 2 * HEAD_WIDTH
QUERY_PER_KEY = 3
NEG_LARGE = -1e30
MESH = pl.DeviceIdType.MESH
LOG2E = math.log2(math.e)
SCORE_BYTES = 30 * 2**20
SUM_LAG = 2
REDUCE_LAG = 5


def dot(a, b, contract):
    return lax.dot_general(a, b, ((contract[:1], contract[1:]), ((), ())), preferred_element_type=jnp.float32)


def kernel(kv_heads, resident, q_far, k_far, v_far, o_far, g_far, dq_in, dkv_in,
           q_ref, k_ref, v_ref, o_ref, g_ref, qg_send, kv_send, dl_send, qg_in, kv_in, dl_in, q_pad, g_pad, dl_row, s0_ref, s1_ref, p0_ref, p1_ref, ds0_ref, ds1_ref, m_ref, dqt_ref,
           acc_ref, dq_send, mate_in, part_ref, red_in, fin_ref,
           in_s, qg_s, qg_r, kv_s, kv_r, dl_s, dl_r, side_s, hand_s, dq_s, dq_r, mate_s, mate_r, red_s, red_r, fin_s, fin_r):
    seq_count = lax.axis_size("seq")
    seq = lax.axis_index("seq")
    span = lax.axis_index("span")
    heads = QUERY_PER_KEY
    spread = lax.axis_size("span") // kv_heads
    splits = spread * seq_count
    tokens = q_far.shape[1]
    per = kv_heads // 2
    chunk = per * tokens
    top = 2 * splits - 1
    me = span * seq_count + seq
    my_head = span // spread
    my_split = lax.rem(span, spread) * seq_count + seq
    scaling = 1.0 / math.sqrt(HEAD_WIDTH)
    factor = scaling * LOG2E

    def rank_of(split):
        return 2 * lax.rem(split, splits // 2) + split // (splits // 2)

    def split_of(rank):
        return lax.rem(rank, 2) * (splits // 2) + rank // 2

    my_rank = rank_of(my_split)
    my_chunk = me // per
    my_kind = jnp.where(my_chunk < splits, 0, 1)
    my_sub = lax.rem(me, per)
    q_split = split_of(jnp.where(my_chunk < splits, my_chunk, top - my_chunk))

    def far(a, t):
        turned, unit = 0, 1
        while unit < kv_heads:
            turned += lax.rem(a // unit + t // unit, 2) * unit
            unit *= 2
        return turned

    def chunk_of(kind):
        return top - my_rank if kind else my_rank

    def member(head, split):
        return {"seq": lax.rem(split, seq_count), "span": head * spread + split // seq_count}

    def source(piece):
        return {"seq": lax.rem(piece, seq_count), "span": piece // seq_count}

    def remote(src, dst, send, recv, device):
        return pltpu.make_async_remote_copy(src_ref=src, dst_ref=dst, send_sem=send, recv_sem=recv,
                                            device_id=device, device_id_type=MESH)

    def other(mine, fn_other, fn_mine):
        @pl.when(mine)
        def _():
            fn_mine()

        @pl.when(jnp.logical_not(mine))
        def _():
            fn_other()

    def qg_copy(h, j):
        return remote(qg_send.at[h, j], qg_in.at[my_kind, j, my_sub], qg_s.at[h, j], qg_r.at[my_kind, j, my_sub],
                      member(h, q_split))

    def qg_own(h, j):
        return pltpu.make_async_copy(qg_send.at[h, j], qg_in.at[my_kind, j, my_sub], qg_s.at[h, j])

    def dl_copy(h):
        return remote(dl_send.at[h], dl_in.at[my_kind, my_sub], dl_s.at[h], dl_r.at[my_kind, my_sub],
                      member(h, q_split))

    def dl_own(h):
        return pltpu.make_async_copy(dl_send.at[h], dl_in.at[my_kind, my_sub], dl_s.at[h])

    def q_mine(h):
        return jnp.logical_and(h == my_head, q_split == my_split)

    def kv_copy(h):
        return remote(kv_send.at[h], kv_in.at[me], kv_s.at[h], kv_r.at[me], member(h, my_split))

    def kv_own(h):
        return pltpu.make_async_copy(kv_send.at[h], kv_in.at[me], kv_s.at[h])

    twin = my_split + 1 - 2 * lax.rem(my_split, 2)

    def step_split(k):
        return lax.rem(my_split + 2 * k, splits)

    def hand_copy(i, k):
        piece = i * splits + my_split
        return remote(kv_in.at[piece], kv_in.at[piece], hand_s.at[k, i], kv_r.at[piece],
                      member(my_head, step_split(k)))

    def twin_copy(i, k):
        piece = i * splits + step_split(k)
        return remote(kv_in.at[piece], kv_in.at[piece], side_s.at[k, i], kv_r.at[piece], member(my_head, twin))

    def kv_wait(piece):
        remote(kv_in.at[piece], kv_in.at[piece], kv_s.at[0], kv_r.at[piece], member(my_head, twin)).wait_recv()

    def dq_copy(kind, j, sub):
        piece = chunk_of(kind) * per + sub
        return remote(dq_send.at[kind, j, sub], dq_in.at[my_head, j], dq_s.at[kind, j, sub], dq_r.at[my_head, j],
                      source(piece))

    def dq_own(kind, j, sub):
        return pltpu.make_async_copy(dq_send.at[kind, j, sub], dq_in.at[my_head, j], dq_s.at[kind, j, sub])

    def has(split, b):
        return top - rank_of(split) >= b

    side = lax.rem(my_split, 2)

    def mate_copy(b, u):
        at = pl.ds(pl.multiple_of((2 * u + 1 - side) * tokens, tokens), tokens)
        return remote(acc_ref.at[b, at, :], mate_in.at[b, u], mate_s.at[b, u], mate_r.at[b, u],
                      member(my_head, twin))

    def mate_wait(b, u):
        landing = mate_in.at[b, u]
        remote(landing, landing, mate_s.at[b, u], mate_r.at[b, u], member(my_head, twin)).wait_recv()

    def red_copy(piece):
        return remote(part_ref.at[piece], red_in.at[my_split // 2, piece // splits], red_s.at[piece],
                      red_r.at[my_split // 2, piece // splits], member(my_head, lax.rem(piece, splits)))

    def fin_copy(i):
        return remote(fin_ref.at[i], dkv_in.at[my_head], fin_s.at[i], fin_r.at[my_head],
                      source(i * splits + my_split))

    def fin_own(i):
        return pltpu.make_async_copy(fin_ref.at[i], dkv_in.at[my_head], fin_s.at[i])

    barrier = pltpu.get_barrier_semaphore()
    everyone = lax.axis_size("span") * seq_count

    def greet(d, _):
        @pl.when(d != me)
        def _():
            pl.semaphore_signal(barrier, inc=1, device_id=source(d), device_id_type=MESH)
        return 0

    lax.fori_loop(0, everyone, greet, 0)

    loads = [pltpu.make_async_copy(far_one, near_one, in_s.at[n]) for n, (far_one, near_one) in enumerate(
        ((k_far, k_ref), (v_far, v_ref), (q_far, q_ref), (g_far, g_ref), (o_far, o_ref)))]
    for load in loads:
        load.start()

    def clear(b, _):
        acc_ref[b] = jnp.zeros((chunk, PAIR), jnp.float32)
        return 0

    lax.fori_loop(0, 2 * splits, clear, 0)
    for load in loads:
        load.wait()

    for h in range(kv_heads):
        at = slice(h * HEAD_WIDTH, (h + 1) * HEAD_WIDTH)
        kv_send[h] = jnp.concatenate([k_ref[0, :, at], v_ref[0, :, at]], axis=1)
    for h in range(kv_heads):
        for j in range(heads):
            one = h * heads + j
            at = slice(one * HEAD_WIDTH, (one + 1) * HEAD_WIDTH)
            qg_send[h, j] = jnp.concatenate([q_ref[0, :, at], g_ref[0, :, at]], axis=1)
    product = o_ref[0].astype(jnp.float32) * g_ref[0].astype(jnp.float32)
    high = product.astype(jnp.bfloat16)
    low = (product - high.astype(jnp.float32)).astype(jnp.bfloat16)
    wide = kv_heads * heads * HEAD_WIDTH
    row = lax.broadcasted_iota(jnp.int32, (kv_heads * 8, wide), 0)
    column = lax.broadcasted_iota(jnp.int32, (kv_heads * 8, wide), 1) // HEAD_WIDTH
    ones = jnp.where(row == (column // heads) * 8 + lax.rem(column, heads), 1.0, 0.0).astype(jnp.bfloat16)
    dl_send[...] = (dot(ones, high, (1, 1)) + dot(ones, low, (1, 1))).reshape(kv_heads, 8, tokens)

    pl.semaphore_wait(barrier, everyone - 1)

    def qg_start(j):
        for t in range(kv_heads):
            h = far(my_head, t)
            other(q_mine(h), lambda: qg_copy(h, j).start(), lambda: qg_own(h, j).start())

    for t in range(kv_heads):
        h = far(my_head, t)
        other(h == my_head, lambda: kv_copy(h).start(), lambda: kv_own(h).start())
    qg_start(0)
    for t in range(kv_heads):
        h = far(my_head, t)
        other(q_mine(h), lambda: dl_copy(h).start(), lambda: dl_own(h).start())

    def hand_on(t, _):
        i = far(my_head, t)
        piece = i * splits + my_split
        other(piece == me, lambda: kv_wait(piece), lambda: kv_own(my_head).wait())
        twin_copy(i, 0).start()
        for k in range(1, splits // 2):
            hand_copy(i, k).start()
        return 0

    lax.fori_loop(0, kv_heads, hand_on, 0)

    def pass_on(i, _):
        for k in range(1, splits // 2):
            kv_wait(i * splits + step_split(k))
            twin_copy(i, k).start()
        return 0

    lax.fori_loop(0, kv_heads, pass_on, 0)

    def twin_wait(i, _):
        for k in range(splits // 2):
            kv_wait(i * splits + lax.rem(twin + 2 * k, splits))
        return 0

    lax.fori_loop(0, kv_heads, twin_wait, 0)

    lane = lax.broadcasted_iota(jnp.int32, (1, PAIR), 1)

    half = chunk // 2
    s_refs = (s0_ref, s1_ref)
    p_refs = (p0_ref, p1_ref)
    ds_refs = (ds0_ref, ds1_ref)

    def kv_half(b, side_of):
        return kv_in[pl.ds(b * per + side_of * (per // 2), per // 2)].reshape(half, PAIR)

    def hide(s):
        k_pos = lax.broadcasted_iota(jnp.int32, s.shape, 0)
        q_pos = lax.broadcasted_iota(jnp.int32, s.shape, 1)
        return jnp.where(k_pos <= q_pos, s, NEG_LARGE)

    def scores(kind, j, b, side_of):
        return dot(kv_half(b, side_of), q_pad[kind, j], (1, 1))

    def top_of(s):
        return jnp.max(s, axis=0, keepdims=True)

    def slot(kind, b):
        return (my_rank + 1) * kind + b if resident else 0

    def stats(kind, j):
        c_q = chunk_of(kind)
        for sub in range(per):
            mine = c_q * per + sub == me
            landing = qg_in.at[kind, j, sub]
            other(mine,
                  lambda: remote(landing, landing, qg_s.at[0, j], qg_r.at[kind, j, sub],
                                 member(my_head, twin)).wait_recv(),
                  lambda: qg_own(my_head, j).wait())
        both = qg_in[kind, j].reshape(chunk, PAIR)
        q_pad[kind, j] = jnp.where(lane < HEAD_WIDTH, both, jnp.zeros_like(both))
        g_pad[kind, j] = jnp.where(lane < HEAD_WIDTH, jnp.zeros_like(both), both)
        dqt_ref[kind, j] = jnp.zeros((HEAD_WIDTH, chunk), jnp.float32)

        def make(b, side_of):
            s = scores(kind, j, b, side_of)
            s_refs[side_of][slot(kind, b)] = s
            return top_of(s)

        def take(b, side_of, seen, m_old, l_old):
            m_new = jnp.maximum(m_old, seen)
            e = jnp.exp2((s_refs[side_of][slot(kind, b)] - m_new) * factor)
            l_new = l_old * jnp.exp2((m_old - m_new) * factor) + jnp.sum(e, axis=0, keepdims=True)
            return m_new, l_new

        def block(b, carry):
            seen, m, l = carry
            later = make(b, 1)
            m, l = take(b, 0, seen, m, l)
            following = make(b + 1, 0)
            m, l = take(b, 1, later, m, l)
            return following, m, l

        start = (make(0, 0), jnp.full((1, chunk), NEG_LARGE, jnp.float32), jnp.zeros((1, chunk), jnp.float32))
        _, m, l = lax.fori_loop(0, c_q, block, start)
        s = hide(s_refs[0][slot(kind, c_q)])
        s_refs[0][slot(kind, c_q)] = s
        m, l = take(c_q, 0, top_of(s), m, l)
        s = hide(dot(kv_half(c_q, 1), q_pad[kind, j, half:], (1, 1)))
        s_refs[1][slot(kind, c_q), :, half:] = s
        m_new = jnp.maximum(m, jnp.concatenate([m[:, :half], top_of(s)], axis=1))
        e = jnp.sum(jnp.exp2((s - m_new[:, half:]) * factor), axis=0, keepdims=True)
        l = l * jnp.exp2((m - m_new) * factor) + jnp.concatenate([jnp.zeros_like(e), e], axis=1)
        m = m_new
        m_ref[kind, j] = m * factor + jnp.log2(l)

    def weigh(kind, j, b, side_of, first=0):
        kv = kv_half(b, side_of)
        if resident:
            s = s_refs[side_of][slot(kind, b), :, first:]
        else:
            s = dot(kv, q_pad[kind, j, first:], (1, 1))
            k_pos = b * chunk + side_of * half + lax.broadcasted_iota(jnp.int32, s.shape, 0)
            q_pos = chunk_of(kind) * chunk + first + lax.broadcasted_iota(jnp.int32, s.shape, 1)
            s = jnp.where(k_pos <= q_pos, s, NEG_LARGE)
        p = jnp.exp2(s * factor - m_ref[kind, j, :, first:])
        dp = dot(kv, g_pad[kind, j, first:], (1, 1))
        ds_refs[side_of][:, first:] = (p * (dp - dl_row[kind, j, :, first:])).astype(jnp.bfloat16)
        p_refs[side_of][:, first:] = p.astype(jnp.bfloat16)
        if first:
            ds_refs[side_of][:, :first] = jnp.zeros((half, first), jnp.bfloat16)
            p_refs[side_of][:, :first] = jnp.zeros((half, first), jnp.bfloat16)

    def gather(kind, j, b, side_of):
        ds = ds_refs[side_of][...]
        at = pl.ds(side_of * half, half)
        acc_ref[b, at, :] += dot(ds, q_pad[kind, j], (1, 0)) + dot(p_refs[side_of][...], g_pad[kind, j], (1, 0))
        dqt_ref[kind, j] += dot(kv_half(b, side_of)[:, :HEAD_WIDTH].T, ds, (1, 0))

    def open_job(kind, j):
        b = chunk_of(kind)
        weigh(kind, j, b, 0)
        weigh(kind, j, b, 1, half)
        gather(kind, j, b, 0)

    def next_block(kind, j, before, b):
        weigh(kind, j, b, 0)
        gather(kind, j, before, 1)
        weigh(kind, j, b, 1)
        gather(kind, j, b, 0)

    def send_dq(kind, j):
        for sub in range(per):
            part = dqt_ref[kind, j, :, sub * tokens:(sub + 1) * tokens] * scaling
            dq_send[kind, j, sub] = part.astype(jnp.bfloat16)
        for sub in range(per):
            other(chunk_of(kind) * per + sub == me, lambda: dq_copy(kind, j, sub).start(),
                  lambda: dq_own(kind, j, sub).start())

    def job(kind, j):
        c_q = chunk_of(kind)
        open_job(kind, j)
        lax.fori_loop(1, c_q + 1, lambda t, _: (next_block(kind, j, c_q - t + 1, c_q - t), 0)[1], 0)
        gather(kind, j, 0, 1)
        send_dq(kind, j)

    weight = jnp.where(lane < HEAD_WIDTH, scaling, 1.0)

    def own_piece(b, u):
        return b * per + 2 * u + side

    def own_rows(u):
        return pl.ds(pl.multiple_of((2 * u + side) * tokens, tokens), tokens)

    def pair_sends(b, u):
        return jnp.logical_and(lax.rem(own_piece(b, u), splits) != my_split,
                               jnp.logical_or(has(my_split, b), has(twin, b)))

    def hand_out(b):
        for u in range(per // 2):
            mate_copy(b, u).start()

    def pair_sum(b):
        @pl.when(has(twin, b))
        def _():
            for u in range(per // 2):
                mate_wait(b, u)
                acc_ref[b, own_rows(u), :] += mate_in[b, u]

        for u in range(per // 2):
            @pl.when(pair_sends(b, u))
            def _():
                piece = own_piece(b, u)
                part_ref[piece] = (acc_ref[b, own_rows(u), :] * weight).astype(jnp.bfloat16)
                red_copy(piece).start()

    def reduce(b):
        for u in range(per // 2):
            piece = own_piece(b, u)

            @pl.when(lax.rem(piece, splits) == my_split)
            def _():
                i = piece // splits
                total = acc_ref.at[b, own_rows(u), :]
                total[...] = total[...] * weight

                def add(f, _):
                    @pl.when(jnp.logical_and(f != my_split // 2,
                                             jnp.logical_or(has(2 * f, b), has(2 * f + 1, b))))
                    def _():
                        landing = red_in.at[f, i]
                        remote(landing, landing, red_s.at[0], red_r.at[f, i], member(my_head, twin)).wait_recv()
                        total[...] += red_in[f, i].astype(jnp.float32)
                    return 0

                lax.fori_loop(0, splits // 2, add, 0)
                fin_ref[i] = total[...].astype(jnp.bfloat16)
                other(piece == me, lambda: fin_copy(i).start(), lambda: fin_own(i).start())

    for kind in range(2):
        c_q = chunk_of(kind)
        for sub in range(per):
            small = dl_in.at[kind, sub]
            other(c_q * per + sub == me,
                  lambda: remote(small, small, dl_s.at[0], dl_r.at[kind, sub], member(my_head, twin)).wait_recv(),
                  lambda: dl_own(my_head).wait())
        for j in range(heads):
            for sub in range(per):
                dl_row[kind, j, :, sub * tokens:(sub + 1) * tokens] = dl_in[kind, sub, pl.ds(j, 1), :]

    def whole_head(j, _):
        stats(0, j)
        qg_start(j + 1)
        stats(1, j)
        for kind in range(2):
            job(kind, j)
        return 0

    lax.fori_loop(0, heads - 1, whole_head, 0)
    final = heads - 1
    for kind in range(2):
        stats(kind, final)
    job(0, final)

    def turn(t):
        return jnp.where(t < splits, top - t, lax.rem(t + my_head, splits))

    def tidy(t, _):
        @pl.when(t >= SUM_LAG)
        def _():
            pair_sum(turn(t - SUM_LAG))

        @pl.when(t >= REDUCE_LAG)
        def _():
            reduce(turn(t - REDUCE_LAG))
        return 0

    def sweep(t, _):
        next_block(1, final, turn(t - 1), turn(t))
        hand_out(turn(t - 1))
        return tidy(t, 0)

    def late_sum(t, _):
        pair_sum(turn(t))
        return 0

    def late_reduce(t, _):
        reduce(turn(t))
        return 0

    lax.fori_loop(0, my_rank + 1, tidy, 0)
    open_job(1, final)
    lax.fori_loop(my_rank + 1, top + 1, sweep, 0)
    gather(1, final, turn(top), 1)
    hand_out(turn(top))
    send_dq(1, final)
    middle = top + 1 - SUM_LAG
    start = max(0, top + 1 - REDUCE_LAG)
    lax.fori_loop(start, middle, late_reduce, 0)
    lax.fori_loop(middle, top + 1, late_sum, 0)
    lax.fori_loop(middle, top + 1, late_reduce, 0)

    for h in range(kv_heads):
        @pl.when(h != my_head)
        def _():
            kv_copy(h).wait_send()

        @pl.when(jnp.logical_not(q_mine(h)))
        def _():
            dl_copy(h).wait_send()
            for j in range(heads):
                qg_copy(h, j).wait_send()

    def sent(i, _):
        for k in range(splits // 2):
            twin_copy(i, k).wait_send()
            if k:
                hand_copy(i, k).wait_send()

        @pl.when(i != my_head)
        def _():
            fin_copy(i).wait_send()
        return 0

    lax.fori_loop(0, kv_heads, sent, 0)
    for kind in range(2):
        for j in range(heads):
            for sub in range(per):
                @pl.when(chunk_of(kind) * per + sub != me)
                def _():
                    dq_copy(kind, j, sub).wait_send()

    def red_sent(b, _):
        for u in range(per // 2):
            @pl.when(has(my_split, b))
            def _():
                mate_copy(b, u).wait_send()

            @pl.when(pair_sends(b, u))
            def _():
                red_copy(own_piece(b, u)).wait_send()
        return 0

    lax.fori_loop(0, top + 1, red_sent, 0)

    for h in range(kv_heads):
        for j in range(heads):
            mine = q_mine(h)
            landing = dq_in.at[h, j]
            other(mine,
                  lambda: remote(landing, landing, dq_s.at[0, j, 0], dq_r.at[h, j], member(my_head, twin)).wait_recv(),
                  lambda: dq_own(my_kind, j, my_sub).wait())
    for h in range(kv_heads):
        landing = dkv_in.at[h]
        other(h == my_head,
              lambda: remote(landing, landing, fin_s.at[0], fin_r.at[h], member(my_head, twin)).wait_recv(),
              lambda: fin_own(my_head).wait())


def results(dq_in, dkv_in, dq_out, dk_out, dv_out):
    kv_heads, heads, _, tokens = dq_in.shape
    dq_out[0] = dq_in[...].reshape(kv_heads * heads * HEAD_WIDTH, tokens).T
    for h in range(0, kv_heads, 2):
        at = slice(h * HEAD_WIDTH, (h + 2) * HEAD_WIDTH)
        dk_out[0, :, at] = jnp.concatenate([dkv_in[h, :, :HEAD_WIDTH], dkv_in[h + 1, :, :HEAD_WIDTH]], axis=1)
        dv_out[0, :, at] = jnp.concatenate([dkv_in[h, :, HEAD_WIDTH:], dkv_in[h + 1, :, HEAD_WIDTH:]], axis=1)


def vmem(count):
    return [pl.BlockSpec(memory_space=pltpu.VMEM)] * count


def per_device(queries, key_head_matrix, value_head_matrix, attn_output, out_grad):
    seq_count = lax.axis_size("seq")
    tokens = queries.shape[1]
    kv_heads = key_head_matrix.shape[2] // HEAD_WIDTH
    splits = lax.axis_size("span") // kv_heads * seq_count
    pieces = kv_heads * splits
    heads = QUERY_PER_KEY
    per = kv_heads // 2
    chunk = per * tokens
    count = 2 * splits + 1
    resident = count * chunk * chunk * 4 <= SCORE_BYTES
    count = count if resident else 1
    dma = pltpu.SemaphoreType.DMA
    low, full = jnp.bfloat16, jnp.float32
    dq, dkv = pl.pallas_call(
        functools.partial(kernel, kv_heads, resident),
        out_shape=(
            jax.ShapeDtypeStruct((kv_heads, heads, HEAD_WIDTH, tokens), low),
            jax.ShapeDtypeStruct((kv_heads, tokens, PAIR), low),
        ),
        in_specs=[pl.BlockSpec(memory_space=pl.ANY)] * 5,
        out_specs=tuple(vmem(2)),
        scratch_shapes=[
            pltpu.VMEM(queries.shape, low),
            pltpu.VMEM(key_head_matrix.shape, low),
            pltpu.VMEM(key_head_matrix.shape, low),
            pltpu.VMEM(queries.shape, low),
            pltpu.VMEM(queries.shape, low),
            pltpu.VMEM((kv_heads, heads, tokens, PAIR), low),
            pltpu.VMEM((kv_heads, tokens, PAIR), low),
            pltpu.VMEM((kv_heads, 8, tokens), full),
            pltpu.VMEM((2, heads, per, tokens, PAIR), low),
            pltpu.VMEM((pieces, tokens, PAIR), low),
            pltpu.VMEM((2, per, 8, tokens), full),
            pltpu.VMEM((2, heads, chunk, PAIR), low),
            pltpu.VMEM((2, heads, chunk, PAIR), low),
            pltpu.VMEM((2, heads, 1, chunk), full),
            pltpu.VMEM((count, chunk // 2, chunk), full),
            pltpu.VMEM((count, chunk // 2, chunk), full),
            pltpu.VMEM((chunk // 2, chunk), low),
            pltpu.VMEM((chunk // 2, chunk), low),
            pltpu.VMEM((chunk // 2, chunk), low),
            pltpu.VMEM((chunk // 2, chunk), low),
            pltpu.VMEM((2, heads, 1, chunk), full),
            pltpu.VMEM((2, heads, HEAD_WIDTH, chunk), full),
            pltpu.VMEM((2 * splits, chunk, PAIR), full),
            pltpu.VMEM((2, heads, per, HEAD_WIDTH, tokens), low),
            pltpu.VMEM((2 * splits, per // 2, tokens, PAIR), full),
            pltpu.VMEM((pieces, tokens, PAIR), low),
            pltpu.VMEM((splits // 2, kv_heads, tokens, PAIR), low),
            pltpu.VMEM((kv_heads, tokens, PAIR), low),
            dma((5,)),
            dma((kv_heads, heads + 1)),
            dma((2, heads + 1, per)),
            dma((kv_heads,)),
            dma((pieces,)),
            dma((kv_heads,)),
            dma((2, per)),
            dma((splits // 2, kv_heads)),
            dma((splits // 2, kv_heads)),
            dma((2, heads, per)),
            dma((kv_heads, heads)),
            dma((2 * splits, per // 2)),
            dma((2 * splits, per // 2)),
            dma((pieces,)),
            dma((splits // 2, kv_heads)),
            dma((kv_heads,)),
            dma((kv_heads,)),
        ],
        compiler_params=pltpu.CompilerParams(collective_id=0, has_side_effects=True, vmem_limit_bytes=60 * 2**20),
        name="attention_grads",
    )(queries, key_head_matrix, value_head_matrix, attn_output, out_grad)
    return pl.pallas_call(
        results,
        out_shape=(
            jax.ShapeDtypeStruct(queries.shape, low),
            jax.ShapeDtypeStruct(key_head_matrix.shape, low),
            jax.ShapeDtypeStruct(value_head_matrix.shape, low),
        ),
        in_specs=vmem(2),
        out_specs=tuple(vmem(3)),
        name="results",
    )(dq, dkv)


def solution(mesh):
    spec = P("span", "seq", None)
    return jax.shard_map(
        per_device, mesh=mesh, in_specs=(spec,) * 5, out_specs=(spec,) * 3, check_vma=False
    )
```

```python
import functools
import math

import jax
import jax.numpy as jnp
from jax import lax
from jax.experimental import pallas as pl
from jax.experimental.pallas import tpu as pltpu
from jax.sharding import PartitionSpec as P

HEAD_WIDTH = 64
PAIR = 2 * HEAD_WIDTH
QUERY_PER_KEY = 3
NEG_LARGE = -1e30
MESH = pl.DeviceIdType.MESH
LOG2E = math.log2(math.e)
SCORE_BYTES = 30 * 2**20
SUM_LAG = 2
REDUCE_LAG = 5


def dot(a, b, contract):
    return lax.dot_general(a, b, ((contract[:1], contract[1:]), ((), ())), preferred_element_type=jnp.float32)


def kernel(kv_heads, resident, q_far, k_far, v_far, o_far, g_far, dq_in, dkv_in,
           q_ref, k_ref, v_ref, o_ref, g_ref, qg_send, kv_send, dl_send, qg_in, kv_in, dl_in, q_pad, g_pad, dl_row, s0_ref, s1_ref, p0_ref, p1_ref, ds0_ref, ds1_ref, m_ref, dqt_ref,
           acc_ref, dq_send, mate_in, part_ref, red_in, fin_ref,
           in_s, qg_s, qg_r, kv_s, kv_r, dl_s, dl_r, side_s, hand_s, dq_s, dq_r, mate_s, mate_r, red_s, red_r, fin_s, fin_r):
    seq_count = lax.axis_size("seq")
    seq = lax.axis_index("seq")
    span = lax.axis_index("span")
    heads = QUERY_PER_KEY
    spread = lax.axis_size("span") // kv_heads
    splits = spread * seq_count
    tokens = q_far.shape[1]
    per = kv_heads // 2
    chunk = per * tokens
    top = 2 * splits - 1
    me = span * seq_count + seq
    my_head = span // spread
    my_split = lax.rem(span, spread) * seq_count + seq
    scaling = 1.0 / math.sqrt(HEAD_WIDTH)
    factor = scaling * LOG2E

    def rank_of(split):
        return 2 * lax.rem(split, splits // 2) + split // (splits // 2)

    def split_of(rank):
        return lax.rem(rank, 2) * (splits // 2) + rank // 2

    my_rank = rank_of(my_split)
    my_chunk = me // per
    my_kind = jnp.where(my_chunk < splits, 0, 1)
    my_sub = lax.rem(me, per)
    q_split = split_of(jnp.where(my_chunk < splits, my_chunk, top - my_chunk))

    def far(a, t):
        turned, unit = 0, 1
        while unit < kv_heads:
            turned += lax.rem(a // unit + t // unit, 2) * unit
            unit *= 2
        return turned

    def chunk_of(kind):
        return top - my_rank if kind else my_rank

    def member(head, split):
        return {"seq": lax.rem(split, seq_count), "span": head * spread + split // seq_count}

    def source(piece):
        return {"seq": lax.rem(piece, seq_count), "span": piece // seq_count}

    def remote(src, dst, send, recv, device):
        return pltpu.make_async_remote_copy(src_ref=src, dst_ref=dst, send_sem=send, recv_sem=recv,
                                            device_id=device, device_id_type=MESH)

    def other(mine, fn_other, fn_mine):
        @pl.when(mine)
        def _():
            fn_mine()

        @pl.when(jnp.logical_not(mine))
        def _():
            fn_other()

    def qg_copy(h, j):
        return remote(qg_send.at[h, j], qg_in.at[my_kind, j, my_sub], qg_s.at[h, j], qg_r.at[my_kind, j, my_sub],
                      member(h, q_split))

    def qg_own(h, j):
        return pltpu.make_async_copy(qg_send.at[h, j], qg_in.at[my_kind, j, my_sub], qg_s.at[h, j])

    def dl_copy(h):
        return remote(dl_send.at[h], dl_in.at[my_kind, my_sub], dl_s.at[h], dl_r.at[my_kind, my_sub],
                      member(h, q_split))

    def dl_own(h):
        return pltpu.make_async_copy(dl_send.at[h], dl_in.at[my_kind, my_sub], dl_s.at[h])

    def q_mine(h):
        return jnp.logical_and(h == my_head, q_split == my_split)

    def kv_copy(h):
        return remote(kv_send.at[h], kv_in.at[me], kv_s.at[h], kv_r.at[me], member(h, my_split))

    def kv_own(h):
        return pltpu.make_async_copy(kv_send.at[h], kv_in.at[me], kv_s.at[h])

    twin = my_split + 1 - 2 * lax.rem(my_split, 2)

    def step_split(k):
        return lax.rem(my_split + 2 * k, splits)

    def hand_copy(i, k):
        piece = i * splits + my_split
        return remote(kv_in.at[piece], kv_in.at[piece], hand_s.at[k, i], kv_r.at[piece],
                      member(my_head, step_split(k)))

    def twin_copy(i, k):
        piece = i * splits + step_split(k)
        return remote(kv_in.at[piece], kv_in.at[piece], side_s.at[k, i], kv_r.at[piece], member(my_head, twin))

    def kv_wait(piece):
        remote(kv_in.at[piece], kv_in.at[piece], kv_s.at[0], kv_r.at[piece], member(my_head, twin)).wait_recv()

    def dq_copy(kind, j, sub):
        piece = chunk_of(kind) * per + sub
        return remote(dq_send.at[kind, j, sub], dq_in.at[my_head, j], dq_s.at[kind, j, sub], dq_r.at[my_head, j],
                      source(piece))

    def dq_own(kind, j, sub):
        return pltpu.make_async_copy(dq_send.at[kind, j, sub], dq_in.at[my_head, j], dq_s.at[kind, j, sub])

    def has(split, b):
        return top - rank_of(split) >= b

    side = lax.rem(my_split, 2)

    def mate_copy(b, u):
        at = pl.ds(pl.multiple_of((2 * u + 1 - side) * tokens, tokens), tokens)
        return remote(acc_ref.at[b, at, :], mate_in.at[b, u], mate_s.at[b, u], mate_r.at[b, u],
                      member(my_head, twin))

    def mate_wait(b, u):
        landing = mate_in.at[b, u]
        remote(landing, landing, mate_s.at[b, u], mate_r.at[b, u], member(my_head, twin)).wait_recv()

    def red_copy(piece):
        return remote(part_ref.at[piece], red_in.at[my_split // 2, piece // splits], red_s.at[piece],
                      red_r.at[my_split // 2, piece // splits], member(my_head, lax.rem(piece, splits)))

    def fin_copy(i):
        return remote(fin_ref.at[i], dkv_in.at[my_head], fin_s.at[i], fin_r.at[my_head],
                      source(i * splits + my_split))

    def fin_own(i):
        return pltpu.make_async_copy(fin_ref.at[i], dkv_in.at[my_head], fin_s.at[i])

    barrier = pltpu.get_barrier_semaphore()
    everyone = lax.axis_size("span") * seq_count

    def greet(d, _):
        @pl.when(d != me)
        def _():
            pl.semaphore_signal(barrier, inc=1, device_id=source(d), device_id_type=MESH)
        return 0

    lax.fori_loop(0, everyone, greet, 0)

    loads = [pltpu.make_async_copy(far_one, near_one, in_s.at[n]) for n, (far_one, near_one) in enumerate(
        ((k_far, k_ref), (v_far, v_ref), (q_far, q_ref), (g_far, g_ref), (o_far, o_ref)))]
    for load in loads:
        load.start()

    def clear(b, _):
        acc_ref[b] = jnp.zeros((chunk, PAIR), jnp.float32)
        return 0

    lax.fori_loop(0, 2 * splits, clear, 0)
    for load in loads:
        load.wait()

    for h in range(kv_heads):
        at = slice(h * HEAD_WIDTH, (h + 1) * HEAD_WIDTH)
        kv_send[h] = jnp.concatenate([k_ref[0, :, at], v_ref[0, :, at]], axis=1)
    for h in range(kv_heads):
        for j in range(heads):
            one = h * heads + j
            at = slice(one * HEAD_WIDTH, (one + 1) * HEAD_WIDTH)
            qg_send[h, j] = jnp.concatenate([q_ref[0, :, at], g_ref[0, :, at]], axis=1)
    product = o_ref[0].astype(jnp.float32) * g_ref[0].astype(jnp.float32)
    high = product.astype(jnp.bfloat16)
    low = (product - high.astype(jnp.float32)).astype(jnp.bfloat16)
    wide = kv_heads * heads * HEAD_WIDTH
    row = lax.broadcasted_iota(jnp.int32, (kv_heads * 8, wide), 0)
    column = lax.broadcasted_iota(jnp.int32, (kv_heads * 8, wide), 1) // HEAD_WIDTH
    ones = jnp.where(row == (column // heads) * 8 + lax.rem(column, heads), 1.0, 0.0).astype(jnp.bfloat16)
    dl_send[...] = (dot(ones, high, (1, 1)) + dot(ones, low, (1, 1))).reshape(kv_heads, 8, tokens)

    pl.semaphore_wait(barrier, everyone - 1)

    def qg_start(j):
        for t in range(kv_heads):
            h = far(my_head, t)
            other(q_mine(h), lambda: qg_copy(h, j).start(), lambda: qg_own(h, j).start())

    for t in range(kv_heads):
        h = far(my_head, t)
        other(h == my_head, lambda: kv_copy(h).start(), lambda: kv_own(h).start())
    qg_start(0)
    for t in range(kv_heads):
        h = far(my_head, t)
        other(q_mine(h), lambda: dl_copy(h).start(), lambda: dl_own(h).start())

    def hand_on(t, _):
        i = far(my_head, t)
        piece = i * splits + my_split
        other(piece == me, lambda: kv_wait(piece), lambda: kv_own(my_head).wait())
        twin_copy(i, 0).start()
        for k in range(1, splits // 2):
            hand_copy(i, k).start()
        return 0

    lax.fori_loop(0, kv_heads, hand_on, 0)

    def pass_on(i, _):
        for k in range(1, splits // 2):
            kv_wait(i * splits + step_split(k))
            twin_copy(i, k).start()
        return 0

    lax.fori_loop(0, kv_heads, pass_on, 0)

    def twin_wait(i, _):
        for k in range(splits // 2):
            kv_wait(i * splits + lax.rem(twin + 2 * k, splits))
        return 0

    lax.fori_loop(0, kv_heads, twin_wait, 0)

    lane = lax.broadcasted_iota(jnp.int32, (1, PAIR), 1)

    half = chunk // 2
    s_refs = (s0_ref, s1_ref)
    p_refs = (p0_ref, p1_ref)
    ds_refs = (ds0_ref, ds1_ref)

    def kv_half(b, side_of):
        return kv_in[pl.ds(b * per + side_of * (per // 2), per // 2)].reshape(half, PAIR)

    def hide(s):
        k_pos = lax.broadcasted_iota(jnp.int32, s.shape, 0)
        q_pos = lax.broadcasted_iota(jnp.int32, s.shape, 1)
        return jnp.where(k_pos <= q_pos, s, NEG_LARGE)

    def scores(kind, j, b, side_of):
        return dot(kv_half(b, side_of), q_pad[kind, j], (1, 1))

    def top_of(s):
        return jnp.max(s, axis=0, keepdims=True)

    def slot(kind, b):
        return (my_rank + 1) * kind + b if resident else 0

    def stats(kind, j):
        c_q = chunk_of(kind)
        for sub in range(per):
            mine = c_q * per + sub == me
            landing = qg_in.at[kind, j, sub]
            other(mine,
                  lambda: remote(landing, landing, qg_s.at[0, j], qg_r.at[kind, j, sub],
                                 member(my_head, twin)).wait_recv(),
                  lambda: qg_own(my_head, j).wait())
        both = qg_in[kind, j].reshape(chunk, PAIR)
        q_pad[kind, j] = jnp.where(lane < HEAD_WIDTH, both, jnp.zeros_like(both))
        g_pad[kind, j] = jnp.where(lane < HEAD_WIDTH, jnp.zeros_like(both), both)
        dqt_ref[kind, j] = jnp.zeros((HEAD_WIDTH, chunk), jnp.float32)

        def make(b, side_of):
            s = scores(kind, j, b, side_of)
            s_refs[side_of][slot(kind, b)] = s
            return top_of(s)

        def take(b, side_of, seen, m_old, l_old):
            m_new = jnp.maximum(m_old, seen)
            e = jnp.exp2((s_refs[side_of][slot(kind, b)] - m_new) * factor)
            l_new = l_old * jnp.exp2((m_old - m_new) * factor) + jnp.sum(e, axis=0, keepdims=True)
            return m_new, l_new

        def block(b, carry):
            seen, m, l = carry
            later = make(b, 1)
            m, l = take(b, 0, seen, m, l)
            following = make(b + 1, 0)
            m, l = take(b, 1, later, m, l)
            return following, m, l

        start = (make(0, 0), jnp.full((1, chunk), NEG_LARGE, jnp.float32), jnp.zeros((1, chunk), jnp.float32))
        _, m, l = lax.fori_loop(0, c_q, block, start)
        s = hide(s_refs[0][slot(kind, c_q)])
        s_refs[0][slot(kind, c_q)] = s
        m, l = take(c_q, 0, top_of(s), m, l)
        s = hide(dot(kv_half(c_q, 1), q_pad[kind, j, half:], (1, 1)))
        s_refs[1][slot(kind, c_q), :, half:] = s
        m_new = jnp.maximum(m, jnp.concatenate([m[:, :half], top_of(s)], axis=1))
        e = jnp.sum(jnp.exp2((s - m_new[:, half:]) * factor), axis=0, keepdims=True)
        l = l * jnp.exp2((m - m_new) * factor) + jnp.concatenate([jnp.zeros_like(e), e], axis=1)
        m = m_new
        m_ref[kind, j] = m * factor + jnp.log2(l)

    def weigh(kind, j, b, side_of, first=0):
        kv = kv_half(b, side_of)
        if resident:
            s = s_refs[side_of][slot(kind, b), :, first:]
        else:
            s = dot(kv, q_pad[kind, j, first:], (1, 1))
            k_pos = b * chunk + side_of * half + lax.broadcasted_iota(jnp.int32, s.shape, 0)
            q_pos = chunk_of(kind) * chunk + first + lax.broadcasted_iota(jnp.int32, s.shape, 1)
            s = jnp.where(k_pos <= q_pos, s, NEG_LARGE)
        p = jnp.exp2(s * factor - m_ref[kind, j, :, first:])
        dp = dot(kv, g_pad[kind, j, first:], (1, 1))
        ds_refs[side_of][:, first:] = (p * (dp - dl_row[kind, j, :, first:])).astype(jnp.bfloat16)
        p_refs[side_of][:, first:] = p.astype(jnp.bfloat16)
        if first:
            ds_refs[side_of][:, :first] = jnp.zeros((half, first), jnp.bfloat16)
            p_refs[side_of][:, :first] = jnp.zeros((half, first), jnp.bfloat16)

    def gather(kind, j, b, side_of):
        ds = ds_refs[side_of][...]
        at = pl.ds(side_of * half, half)
        acc_ref[b, at, :] += dot(ds, q_pad[kind, j], (1, 0)) + dot(p_refs[side_of][...], g_pad[kind, j], (1, 0))
        dqt_ref[kind, j] += dot(kv_half(b, side_of)[:, :HEAD_WIDTH].T, ds, (1, 0))

    def open_job(kind, j):
        b = chunk_of(kind)
        weigh(kind, j, b, 0)
        weigh(kind, j, b, 1, half)
        gather(kind, j, b, 0)

    def next_block(kind, j, before, b):
        weigh(kind, j, b, 0)
        gather(kind, j, before, 1)
        weigh(kind, j, b, 1)
        gather(kind, j, b, 0)

    def send_dq(kind, j):
        for sub in range(per):
            part = dqt_ref[kind, j, :, sub * tokens:(sub + 1) * tokens] * scaling
            dq_send[kind, j, sub] = part.astype(jnp.bfloat16)
        for sub in range(per):
            other(chunk_of(kind) * per + sub == me, lambda: dq_copy(kind, j, sub).start(),
                  lambda: dq_own(kind, j, sub).start())

    def job(kind, j):
        c_q = chunk_of(kind)
        open_job(kind, j)
        lax.fori_loop(1, c_q + 1, lambda t, _: (next_block(kind, j, c_q - t + 1, c_q - t), 0)[1], 0)
        gather(kind, j, 0, 1)
        send_dq(kind, j)

    weight = jnp.where(lane < HEAD_WIDTH, scaling, 1.0)

    def own_piece(b, u):
        return b * per + 2 * u + side

    def own_rows(u):
        return pl.ds(pl.multiple_of((2 * u + side) * tokens, tokens), tokens)

    def pair_sends(b, u):
        return jnp.logical_and(lax.rem(own_piece(b, u), splits) != my_split,
                               jnp.logical_or(has(my_split, b), has(twin, b)))

    def hand_out(b):
        for u in range(per // 2):
            mate_copy(b, u).start()

    def pair_sum(b):
        @pl.when(has(twin, b))
        def _():
            for u in range(per // 2):
                mate_wait(b, u)
                acc_ref[b, own_rows(u), :] += mate_in[b, u]

        for u in range(per // 2):
            @pl.when(pair_sends(b, u))
            def _():
                piece = own_piece(b, u)
                part_ref[piece] = (acc_ref[b, own_rows(u), :] * weight).astype(jnp.bfloat16)
                red_copy(piece).start()

    def reduce(b):
        for u in range(per // 2):
            piece = own_piece(b, u)

            @pl.when(lax.rem(piece, splits) == my_split)
            def _():
                i = piece // splits
                total = acc_ref.at[b, own_rows(u), :]
                total[...] = total[...] * weight

                def add(f, _):
                    @pl.when(jnp.logical_and(f != my_split // 2,
                                             jnp.logical_or(has(2 * f, b), has(2 * f + 1, b))))
                    def _():
                        landing = red_in.at[f, i]
                        remote(landing, landing, red_s.at[0], red_r.at[f, i], member(my_head, twin)).wait_recv()
                        total[...] += red_in[f, i].astype(jnp.float32)
                    return 0

                lax.fori_loop(0, splits // 2, add, 0)
                fin_ref[i] = total[...].astype(jnp.bfloat16)
                other(piece == me, lambda: fin_copy(i).start(), lambda: fin_own(i).start())

    for kind in range(2):
        c_q = chunk_of(kind)
        for sub in range(per):
            small = dl_in.at[kind, sub]
            other(c_q * per + sub == me,
                  lambda: remote(small, small, dl_s.at[0], dl_r.at[kind, sub], member(my_head, twin)).wait_recv(),
                  lambda: dl_own(my_head).wait())
        for j in range(heads):
            for sub in range(per):
                dl_row[kind, j, :, sub * tokens:(sub + 1) * tokens] = dl_in[kind, sub, pl.ds(j, 1), :]

    def whole_head(j, _):
        stats(0, j)
        qg_start(j + 1)
        stats(1, j)
        for kind in range(2):
            job(kind, j)
        return 0

    lax.fori_loop(0, heads - 1, whole_head, 0)
    final = heads - 1
    for kind in range(2):
        stats(kind, final)
    job(0, final)

    def turn(t):
        return jnp.where(t < splits, top - t, lax.rem(t + my_head, splits))

    def tidy(t, _):
        @pl.when(t >= SUM_LAG)
        def _():
            pair_sum(turn(t - SUM_LAG))

        @pl.when(t >= REDUCE_LAG)
        def _():
            reduce(turn(t - REDUCE_LAG))
        return 0

    def sweep(t, _):
        before, b = turn(t - 1), turn(t)
        weigh(1, final, b, 0)
        gather(1, final, before, 1)
        hand_out(before)
        weigh(1, final, b, 1)
        gather(1, final, b, 0)
        return tidy(t, 0)

    def late_sum(t, _):
        pair_sum(turn(t))
        return 0

    def late_reduce(t, _):
        reduce(turn(t))
        return 0

    lax.fori_loop(0, my_rank + 1, tidy, 0)
    open_job(1, final)
    lax.fori_loop(my_rank + 1, top + 1, sweep, 0)
    gather(1, final, turn(top), 1)
    hand_out(turn(top))
    send_dq(1, final)
    middle = top + 1 - SUM_LAG
    start = max(0, top + 1 - REDUCE_LAG)
    lax.fori_loop(middle, top + 1, late_sum, 0)
    lax.fori_loop(start, middle, late_reduce, 0)
    lax.fori_loop(middle, top + 1, late_reduce, 0)

    for h in range(kv_heads):
        @pl.when(h != my_head)
        def _():
            kv_copy(h).wait_send()

        @pl.when(jnp.logical_not(q_mine(h)))
        def _():
            dl_copy(h).wait_send()
            for j in range(heads):
                qg_copy(h, j).wait_send()

    def sent(i, _):
        for k in range(splits // 2):
            twin_copy(i, k).wait_send()
            if k:
                hand_copy(i, k).wait_send()

        @pl.when(i != my_head)
        def _():
            fin_copy(i).wait_send()
        return 0

    lax.fori_loop(0, kv_heads, sent, 0)
    for kind in range(2):
        for j in range(heads):
            for sub in range(per):
                @pl.when(chunk_of(kind) * per + sub != me)
                def _():
                    dq_copy(kind, j, sub).wait_send()

    def red_sent(b, _):
        for u in range(per // 2):
            @pl.when(has(my_split, b))
            def _():
                mate_copy(b, u).wait_send()

            @pl.when(pair_sends(b, u))
            def _():
                red_copy(own_piece(b, u)).wait_send()
        return 0

    lax.fori_loop(0, top + 1, red_sent, 0)

    for h in range(kv_heads):
        for j in range(heads):
            mine = q_mine(h)
            landing = dq_in.at[h, j]
            other(mine,
                  lambda: remote(landing, landing, dq_s.at[0, j, 0], dq_r.at[h, j], member(my_head, twin)).wait_recv(),
                  lambda: dq_own(my_kind, j, my_sub).wait())
    for h in range(kv_heads):
        landing = dkv_in.at[h]
        other(h == my_head,
              lambda: remote(landing, landing, fin_s.at[0], fin_r.at[h], member(my_head, twin)).wait_recv(),
              lambda: fin_own(my_head).wait())


def results(dq_in, dkv_in, dq_out, dk_out, dv_out):
    kv_heads, heads, _, tokens = dq_in.shape
    dq_out[0] = dq_in[...].reshape(kv_heads * heads * HEAD_WIDTH, tokens).T
    for h in range(0, kv_heads, 2):
        at = slice(h * HEAD_WIDTH, (h + 2) * HEAD_WIDTH)
        dk_out[0, :, at] = jnp.concatenate([dkv_in[h, :, :HEAD_WIDTH], dkv_in[h + 1, :, :HEAD_WIDTH]], axis=1)
        dv_out[0, :, at] = jnp.concatenate([dkv_in[h, :, HEAD_WIDTH:], dkv_in[h + 1, :, HEAD_WIDTH:]], axis=1)


def vmem(count):
    return [pl.BlockSpec(memory_space=pltpu.VMEM)] * count


def per_device(queries, key_head_matrix, value_head_matrix, attn_output, out_grad):
    seq_count = lax.axis_size("seq")
    tokens = queries.shape[1]
    kv_heads = key_head_matrix.shape[2] // HEAD_WIDTH
    splits = lax.axis_size("span") // kv_heads * seq_count
    pieces = kv_heads * splits
    heads = QUERY_PER_KEY
    per = kv_heads // 2
    chunk = per * tokens
    count = 2 * splits + 1
    resident = count * chunk * chunk * 4 <= SCORE_BYTES
    count = count if resident else 1
    dma = pltpu.SemaphoreType.DMA
    low, full = jnp.bfloat16, jnp.float32
    dq, dkv = pl.pallas_call(
        functools.partial(kernel, kv_heads, resident),
        out_shape=(
            jax.ShapeDtypeStruct((kv_heads, heads, HEAD_WIDTH, tokens), low),
            jax.ShapeDtypeStruct((kv_heads, tokens, PAIR), low),
        ),
        in_specs=[pl.BlockSpec(memory_space=pl.ANY)] * 5,
        out_specs=tuple(vmem(2)),
        scratch_shapes=[
            pltpu.VMEM(queries.shape, low),
            pltpu.VMEM(key_head_matrix.shape, low),
            pltpu.VMEM(key_head_matrix.shape, low),
            pltpu.VMEM(queries.shape, low),
            pltpu.VMEM(queries.shape, low),
            pltpu.VMEM((kv_heads, heads, tokens, PAIR), low),
            pltpu.VMEM((kv_heads, tokens, PAIR), low),
            pltpu.VMEM((kv_heads, 8, tokens), full),
            pltpu.VMEM((2, heads, per, tokens, PAIR), low),
            pltpu.VMEM((pieces, tokens, PAIR), low),
            pltpu.VMEM((2, per, 8, tokens), full),
            pltpu.VMEM((2, heads, chunk, PAIR), low),
            pltpu.VMEM((2, heads, chunk, PAIR), low),
            pltpu.VMEM((2, heads, 1, chunk), full),
            pltpu.VMEM((count, chunk // 2, chunk), full),
            pltpu.VMEM((count, chunk // 2, chunk), full),
            pltpu.VMEM((chunk // 2, chunk), low),
            pltpu.VMEM((chunk // 2, chunk), low),
            pltpu.VMEM((chunk // 2, chunk), low),
            pltpu.VMEM((chunk // 2, chunk), low),
            pltpu.VMEM((2, heads, 1, chunk), full),
            pltpu.VMEM((2, heads, HEAD_WIDTH, chunk), full),
            pltpu.VMEM((2 * splits, chunk, PAIR), full),
            pltpu.VMEM((2, heads, per, HEAD_WIDTH, tokens), low),
            pltpu.VMEM((2 * splits, per // 2, tokens, PAIR), full),
            pltpu.VMEM((pieces, tokens, PAIR), low),
            pltpu.VMEM((splits // 2, kv_heads, tokens, PAIR), low),
            pltpu.VMEM((kv_heads, tokens, PAIR), low),
            dma((5,)),
            dma((kv_heads, heads + 1)),
            dma((2, heads + 1, per)),
            dma((kv_heads,)),
            dma((pieces,)),
            dma((kv_heads,)),
            dma((2, per)),
            dma((splits // 2, kv_heads)),
            dma((splits // 2, kv_heads)),
            dma((2, heads, per)),
            dma((kv_heads, heads)),
            dma((2 * splits, per // 2)),
            dma((2 * splits, per // 2)),
            dma((pieces,)),
            dma((splits // 2, kv_heads)),
            dma((kv_heads,)),
            dma((kv_heads,)),
        ],
        compiler_params=pltpu.CompilerParams(collective_id=0, has_side_effects=True, vmem_limit_bytes=60 * 2**20),
        name="attention_grads",
    )(queries, key_head_matrix, value_head_matrix, attn_output, out_grad)
    return pl.pallas_call(
        results,
        out_shape=(
            jax.ShapeDtypeStruct(queries.shape, low),
            jax.ShapeDtypeStruct(key_head_matrix.shape, low),
            jax.ShapeDtypeStruct(value_head_matrix.shape, low),
        ),
        in_specs=vmem(2),
        out_specs=tuple(vmem(3)),
        name="results",
    )(dq, dkv)


def solution(mesh):
    spec = P("span", "seq", None)
    return jax.shard_map(
        per_device, mesh=mesh, in_specs=(spec,) * 5, out_specs=(spec,) * 3, check_vma=False
    )
```
